32 devices in a mesh: fsdp: 8 (over z, x), tp: 4 (over y, core).
Axes of the slice: x: 2, y: 2, z: 4, core: 2. Of those that a mesh axis runs over, the one named last changes fastest.
Arguments:
- slopes_in: float32 [32, 128, 4096], P(None, 'fsdp', 'tp'), may hold values from -6 to 6
- moments_in: float32 [32, 128, 4096], P(None, 'fsdp', 'tp'), may hold values from -6 to 6
- weights_in: float32 [32, 128, 4096], P(None, 'fsdp', 'tp'), may hold values from -0.1875 to 0.1875
Outputs:
- new_weights: float32 [32, 128, 4096], P(None, 'fsdp', 'tp')
- new_momentum: float32 [32, 128, 4096], P(None, 'fsdp', 'tp')
The draws below stay inside these ranges and needn't reach their ends.
All inputs are finite; a program needn't handle non-finite values.
Results may differ from the reference program's by a relative error of at most 0.00021.
Values sent between devices are 32-bit elements; how exact they have to be, the bound alone decides.
A program may use at most 128 MiB of HBM per device.

```python
import jax
import jax.numpy as jnp
from jax import lax

SIDE = 128
WIDE = 4096
MATS = 32
ITERS = 5


def level_of(own_key, dims, split, smallest, top_value):
    level, own = 1.0, jax.random.fold_in(own_key, 6)
    for position, parts in split:
        heights = jnp.exp(jax.random.uniform(jax.random.fold_in(own, position), (parts,), jnp.float32, smallest / len(split), top_value / len(split)))
        level = level * jnp.repeat(heights, dims[position] // parts).reshape([-1 if axis == position else 1 for axis in range(len(dims))])
    return level


def normal_values(key, extent, scale, reach, cuts=(), held_as=jnp.bfloat16):
    loudness = level_of(key, extent, cuts, -0.22, 0.18) if cuts else 1.0
    array = jax.random.normal(key, extent, jnp.float32) * scale * loudness
    return jnp.minimum(jnp.maximum(array, -reach), reach).astype(held_as)


def setup_inputs(seed: int = 0) -> dict:
    seeds = jax.random.split(jax.random.key(seed), 4)
    slopes_in = normal_values(seeds[0], (MATS, SIDE, WIDE), 1.0, 6.0, ((1, 8), (2, 4)), jnp.float32)
    moments_in = normal_values(seeds[1], (MATS, SIDE, WIDE), 1.0, 6.0, ((1, 8), (2, 4)), jnp.float32)
    weights_in = normal_values(seeds[2], (MATS, SIDE, WIDE), 0.03, 0.1875, ((1, 8), (2, 4)), jnp.float32)
    return {"slopes_in": slopes_in, "moments_in": moments_in, "weights_in": weights_in}


hold_rate = 0.8
learn_rate = 1.0

def reference(slopes_in, moments_in, weights_in):
    new_momentum = hold_rate * moments_in + slopes_in

    def orthogonal_one(stack):
        iterate = stack[None]
        iterate = iterate * lax.rsqrt(lax.optimization_barrier(jnp.sum(iterate * iterate, axis=(1, 2), keepdims=True)) + 1e-06)
        for step in range(ITERS):
            gram = jnp.einsum('mik,mjk->mij', iterate, iterate, precision=lax.Precision.HIGHEST)
            mixed = -4.775 * gram + 2.0315 * jnp.einsum('mij,mjk->mik', gram, gram, precision=lax.Precision.HIGHEST)
            iterate = 3.4445 * iterate + jnp.einsum('mij,mjk->mik', mixed, iterate, precision=lax.Precision.HIGHEST)
        return iterate[0]
    iterate = lax.map(orthogonal_one, new_momentum)
    new_weights = weights_in - learn_rate * iterate
    return (new_weights, new_momentum)
```

```python
import functools

import jax
import jax.numpy as jnp
from jax import lax
from jax.experimental import pallas as pl
from jax.experimental.pallas import tpu as pltpu
from jax.sharding import PartitionSpec as P

ITERS = 5
HIGH = lax.Precision.HIGHEST
MESH = pl.DeviceIdType.MESH


hold_rate = 0.8
learn_rate = 1.0


def polynomial(gram, dot, trace):
    side = gram.shape[-1]
    eye = jnp.where(
        lax.broadcasted_iota(jnp.int32, (side, side), 0) == lax.broadcasted_iota(jnp.int32, (side, side), 1), 1.0, 0.0
    ).astype(gram.dtype)
    scale = lax.rsqrt(trace(gram * eye) + 1e-06)
    gram = gram * (scale * scale)
    total = None
    for step in range(ITERS):
        mixed = 3.4445 * eye - 4.775 * gram + 2.0315 * dot(gram, gram)
        total = mixed * scale if total is None else dot(mixed, total)
        if step < ITERS - 1:
            gram = dot(dot(mixed, gram), mixed)
    return total


def kernel(
    stages, parts, cols, slopes_ref, moments_ref, weights_ref, momentum_ref, new_ref,
    sm_ref, w_ref, back_ref, x_ref, y_ref, g_ref, loads, wload, fsend, frecv, bsend, brecv, blast, gsend, grecv, rounds,
):
    rows, wide = momentum_ref.shape[1:]
    side, mats, half = parts * rows, stages * parts, parts // 2
    last = stages - 1
    f, t = lax.axis_index("fsdp"), lax.axis_index("tp")
    upper = f // half

    def pair(k):
        peer = f
        for bit in range(k.bit_length()):
            if k >> bit & 1:
                peer = peer + (1 - 2 * ((f // 2**bit) % 2)) * 2**bit
        return peer

    def across(i):
        return upper * i + (1 - upper) * (parts - 1 - i)

    near = [k for k in (parts - 2, 2, 1) if 0 < k < parts]
    far = [k for k in range(parts - 1, 0, -1) if k not in near]

    def load(m, which, src):
        some = pl.ds(m * parts, parts)
        return pltpu.make_async_copy(src.at[some], sm_ref.at[which, some], loads.at[m])

    @pl.loop(0, stages)
    def _(m):
        load(m, 0, slopes_ref).start()
        load(m, 1, moments_ref).start()

    barrier = pltpu.get_barrier_semaphore()
    for k in near:
        pl.semaphore_signal(barrier, inc=1, device_id={"fsdp": pair(k)}, device_id_type=MESH)
    for k in range(1, cols):
        pl.semaphore_signal(barrier, inc=1, device_id={"tp": lax.rem(t + k, cols)}, device_id_type=MESH)

    def forward(m, peer):
        return pltpu.make_async_remote_copy(
            src_ref=momentum_ref.at[m * parts + peer], dst_ref=x_ref.at[m, f],
            send_sem=fsend.at[0], recv_sem=frecv.at[m],
            device_id={"fsdp": peer}, device_id_type=MESH,
        )

    def backward(m, peer, recv):
        return pltpu.make_async_remote_copy(
            src_ref=y_ref.at[m, peer], dst_ref=back_ref.at[m * parts + f],
            send_sem=bsend.at[0], recv_sem=recv,
            device_id={"fsdp": peer}, device_id_type=MESH,
        )

    def partial(m, peer):
        return pltpu.make_async_remote_copy(
            src_ref=g_ref.at[m * cols + t], dst_ref=g_ref.at[m * cols + t],
            send_sem=gsend.at[0], recv_sem=grecv.at[m],
            device_id={"tp": peer}, device_id_type=MESH,
        )

    def settle(ref, sem):
        pltpu.make_async_copy(ref, ref, sem).wait()

    def add(m):
        some = pl.ds(m * parts, parts)
        settle(sm_ref.at[:, some], loads.at[m])
        momentum_ref[some] = hold_rate * sm_ref[1, some] + sm_ref[0, some]
        x_ref[m, f] = hold_rate * sm_ref[1, m * parts + f] + sm_ref[0, m * parts + f]

    def greet(r):
        for k in near:
            pl.semaphore_signal(rounds.at[r], inc=1, device_id={"fsdp": pair(k)}, device_id_type=MESH)

    add(0)
    pl.semaphore_wait(barrier, len(near) + cols - 1)
    forward(0, pair(near[0])).start()
    greet(0)
    for k in near[1:]:
        forward(0, pair(k)).start()

    @pl.loop(1, stages)
    def _(m):
        add(m)
        forward(m, pair(near[0])).start()

    pl.semaphore_wait(rounds.at[0], len(near))
    greet(1)
    for k in far:
        if k != parts - 3:
            forward(0, pair(k)).start()
    pl.semaphore_wait(rounds.at[1], len(near))
    forward(0, pair(parts - 3)).start()

    @pl.loop(1, stages)
    def _(m):
        for k in range(parts - 1, 0, -1):
            if k != near[0]:
                forward(m, pair(k)).start()

    weights = pltpu.make_async_copy(weights_ref, w_ref, wload.at[0])
    weights.start()

    dot = functools.partial(jnp.dot, precision=HIGH, preferred_element_type=jnp.float32)

    @pl.loop(0, stages)
    def _(m):
        settle(x_ref.at[m, pl.ds(0, parts - 1)], frecv.at[m])
        x = x_ref[m].reshape(side, wide)
        g_ref[m * cols + t] = lax.dot_general(x, x, (((1,), (1,)), ((), ())), precision=HIGH, preferred_element_type=jnp.float32)
        for k in range(1, cols):
            partial(m, lax.rem(t + k, cols)).start()
        settle(g_ref.at[pl.ds(m * cols, cols - 1)], grecv.at[m])
        gram = g_ref[m * cols]
        for k in range(1, cols):
            gram = gram + g_ref[m * cols + k]
        total = polynomial(gram, dot, lambda a: jnp.sum(jnp.sum(a, axis=1, keepdims=True), axis=0, keepdims=True))
        y_ref[m] = dot(total, x_ref[m].reshape(side, wide)).reshape(parts, rows, wide)

        @pl.when(m < last)
        def _():
            for i in range(half):
                backward(m, across(i), brecv.at[m]).start()
            for k in range(half - 1, 0, -1):
                backward(m, pair(k), brecv.at[m]).start()

        @pl.when(m == last)
        def _():
            for k in range(half - 1, 0, -1):
                backward(m, pair(k), blast.at[f]).start()
            for i in range(half):
                backward(m, across(i), blast.at[f]).start()

    weights.wait()

    def finish(m, peer):
        mat = m * parts + peer
        new_ref[mat] = w_ref[mat] - learn_rate * back_ref[mat]

    def own(m):
        mat = m * parts + f
        new_ref[mat] = w_ref[mat] - learn_rate * y_ref[m, f]

    @pl.loop(0, last)
    def _(m):
        settle(back_ref.at[pl.ds(0, parts - 1)], brecv.at[m])
        own(m)
        for k in range(1, parts):
            finish(m, pair(k))

    own(last)
    for peer in [*[pair(k) for k in range(half - 1, 0, -1)], *[across(i) for i in range(half)]]:
        settle(back_ref.at[last * parts + peer], blast.at[peer])
        finish(last, peer)

    settle(momentum_ref.at[pl.ds(0, mats - stages)], fsend.at[0])
    settle(back_ref.at[pl.ds(0, mats - stages)], bsend.at[0])
    settle(g_ref.at[pl.ds(0, stages * (cols - 1))], gsend.at[0])


def leave(first_ref, second_ref, first_out, second_out, sems):
    copies = [pltpu.make_async_copy(first_ref, first_out, sems.at[0]), pltpu.make_async_copy(second_ref, second_out, sems.at[1])]
    for copy in copies:
        copy.start()
    for copy in copies:
        copy.wait()


def leave_kernel(first, second):
    return pl.pallas_call(
        leave,
        out_shape=[jax.ShapeDtypeStruct(a.shape, a.dtype) for a in (first, second)],
        in_specs=[pl.BlockSpec(memory_space=pl.ANY)] * 2,
        out_specs=[pl.BlockSpec(memory_space=pl.ANY)] * 2,
        scratch_shapes=[pltpu.SemaphoreType.DMA((2,))],
        compiler_params=pltpu.CompilerParams(vmem_limit_bytes=2**20),
    )(first, second)


def iterate_kernel(slopes_in, moments_in, weights_in, parts, cols):
    mats, rows, wide = slopes_in.shape
    stages, side = mats // parts, rows * parts
    dma = pltpu.SemaphoreType.DMA
    return pl.pallas_call(
        functools.partial(kernel, stages, parts, cols),
        out_shape=[jax.ShapeDtypeStruct(slopes_in.shape, slopes_in.dtype)] * 2,
        in_specs=[pl.BlockSpec(memory_space=pltpu.HBM)] * 3,
        out_specs=[pl.BlockSpec(memory_space=pltpu.VMEM)] * 2,
        scratch_shapes=[
            pltpu.VMEM((2, mats, rows, wide), jnp.float32),
            *[pltpu.VMEM((mats, rows, wide), jnp.float32)] * 2,
            *[pltpu.VMEM((stages, parts, rows, wide), jnp.float32)] * 2,
            pltpu.VMEM((stages * cols, side, side), jnp.float32),
            dma((stages,)), dma((1,)), dma((1,)), dma((stages,)), dma((1,)), dma((stages,)), dma((parts,)),
            dma((1,)), dma((stages,)), pltpu.SemaphoreType.REGULAR((2,)),
        ],
        compiler_params=pltpu.CompilerParams(collective_id=0, has_side_effects=True, vmem_limit_bytes=48 * 2**20),
    )(slopes_in, moments_in, weights_in)


def iterate_plain(new_momentum):
    moved = lax.all_to_all(new_momentum, "fsdp", split_axis=0, concat_axis=1, tiled=True)
    gram = lax.psum(jnp.einsum("mik,mjk->mij", moved, moved, precision=HIGH), "tp")
    dot = functools.partial(jnp.einsum, "mij,mjk->mik", precision=HIGH)
    total = polynomial(gram, dot, lambda a: jnp.sum(a, axis=(1, 2), keepdims=True))
    return lax.all_to_all(dot(total, moved), "fsdp", split_axis=1, concat_axis=0, tiled=True)


def body(parts, cols, slopes_in, moments_in, weights_in):
    if slopes_in.shape[1] % 8 == 0:
        new_momentum, new_weights = iterate_kernel(slopes_in, moments_in, weights_in, parts, cols)
        new_weights, new_momentum = leave_kernel(new_weights, new_momentum)
    else:
        new_momentum = hold_rate * moments_in + slopes_in
        new_weights = weights_in - learn_rate * iterate_plain(new_momentum)
    return (new_weights, new_momentum)


def solution(mesh):
    return jax.shard_map(
        functools.partial(body, mesh.shape["fsdp"], mesh.shape["tp"]),
        mesh=mesh,
        in_specs=(P(None, "fsdp", "tp"), P(None, "fsdp", "tp"), P(None, "fsdp", "tp")),
        out_specs=(P(None, "fsdp", "tp"), P(None, "fsdp", "tp")),
        check_vma=False,
    )
```

```python
import functools

import jax
import jax.numpy as jnp
from jax import lax
from jax.experimental import pallas as pl
from jax.experimental.pallas import tpu as pltpu
from jax.sharding import PartitionSpec as P

ITERS = 5
HIGH = lax.Precision.HIGHEST
MESH = pl.DeviceIdType.MESH


hold_rate = 0.8
learn_rate = 1.0


def polynomial(gram, dot, trace):
    side = gram.shape[-1]
    eye = jnp.where(
        lax.broadcasted_iota(jnp.int32, (side, side), 0) == lax.broadcasted_iota(jnp.int32, (side, side), 1), 1.0, 0.0
    ).astype(gram.dtype)
    scale = lax.rsqrt(trace(gram * eye) + 1e-06)
    gram = gram * (scale * scale)
    total = None
    for step in range(ITERS):
        mixed = 3.4445 * eye - 4.775 * gram + 2.0315 * dot(gram, gram)
        total = mixed * scale if total is None else dot(mixed, total)
        if step < ITERS - 1:
            gram = dot(dot(mixed, gram), mixed)
    return total


def kernel(
    stages, parts, cols, slopes_ref, moments_ref, weights_ref, momentum_ref, new_ref,
    first_ref, sm_ref, w_ref, back_ref, x_ref, y_ref, g_ref, loads, fsend, frecv, bsend, brecv, blast, gsend, grecv, met, rounds,
):
    rows, wide = momentum_ref.shape[1:]
    side, mats, half, last = parts * rows, stages * parts, parts // 2, stages - 1
    f, t = lax.axis_index("fsdp"), lax.axis_index("tp")
    upper = f // half

    def pair(k):
        peer = f
        for bit in range(k.bit_length()):
            if k >> bit & 1:
                peer = peer + (1 - 2 * ((f // 2**bit) % 2)) * 2**bit
        return peer

    near, level = neighbours(parts)
    n_rounds = max(level.values()) - 1
    if half > 2:
        outer = jnp.where((f // 2 == half // 2 - 1) | (f // 2 == half // 2), 0, 1)
    else:
        outer = f * 0 + 1
    first = near[0]
    rest = [k for k in range(parts - 1, 0, -1) if k != first]
    inside = [pair(k) for k in range(half - 1, 0, -1)]
    outside = []
    for j in range(half // 2):
        z = upper * j + (1 - upper) * (half - 1 - j)
        x = f % 2 if j == half // 2 - 1 else 1
        outside += [2 * z + 1 - x, 2 * z + x]

    def near_signal(sem):
        for k in near:
            pl.semaphore_signal(sem, inc=1, device_id={"fsdp": pair(k)}, device_id_type=MESH)

    def tp_signal(sem):
        @pl.when(outer == 1)
        def _():
            for k in range(1, cols):
                pl.semaphore_signal(sem, inc=1, device_id={"tp": lax.rem(t + k, cols)}, device_id_type=MESH)

    barrier = pltpu.get_barrier_semaphore()

    def load_first(m, sem):
        mat = m * parts + pair(first)
        pltpu.make_async_copy(slopes_ref.at[mat], first_ref.at[0, m], sem).start()
        pltpu.make_async_copy(moments_ref.at[mat], first_ref.at[1, m], sem).start()

    load_first(0, loads.at[0])
    near_signal(barrier)
    for m in range(1, stages):
        load_first(m, loads.at[1])

    tp_signal(barrier)

    def forward(m, peer):
        return pltpu.make_async_remote_copy(
            src_ref=momentum_ref.at[m * parts + peer], dst_ref=x_ref.at[m, f],
            send_sem=fsend.at[0], recv_sem=frecv.at[m],
            device_id={"fsdp": peer}, device_id_type=MESH,
        )

    def backward(m, peer, recv):
        return pltpu.make_async_remote_copy(
            src_ref=y_ref.at[m, peer], dst_ref=back_ref.at[m * parts + f],
            send_sem=bsend.at[0], recv_sem=recv,
            device_id={"fsdp": peer}, device_id_type=MESH,
        )

    def partial(m, peer):
        return pltpu.make_async_remote_copy(
            src_ref=g_ref.at[m * cols + t], dst_ref=g_ref.at[m * cols + t],
            send_sem=gsend.at[0], recv_sem=grecv.at[lax.rem(m, 2)],
            device_id={"tp": peer}, device_id_type=MESH,
        )

    def settle(ref, sem):
        pltpu.make_async_copy(ref, ref, sem).wait()

    def add(m):
        for k in [0, *rest]:
            mat = m * parts + pair(k)
            value = hold_rate * sm_ref[1, mat] + sm_ref[0, mat]
            momentum_ref[mat] = value
            if k == 0:
                x_ref[m, f] = value

    settle(first_ref.at[:, 0], loads.at[0])
    momentum_ref[pair(first)] = hold_rate * first_ref[1, 0] + first_ref[0, 0]
    for which, src in enumerate((slopes_ref, moments_ref)):
        pltpu.make_async_copy(src, sm_ref.at[which], loads.at[0]).start()
    pl.semaphore_wait(barrier, len(near) + outer * (cols - 1))
    forward(0, pair(first)).start()
    settle(first_ref.at[:, pl.ds(1, stages - 1)], loads.at[1])
    for m in range(1, stages):
        momentum_ref[m * parts + pair(first)] = hold_rate * first_ref[1, m] + first_ref[0, m]
        forward(m, pair(first)).start()
    tp_signal(met.at[0])
    if n_rounds:
        near_signal(rounds.at[0])
    settle(sm_ref, loads.at[0])
    add(0)
    for k in rest:
        if level[k] == 1:
            forward(0, pair(k)).start()

    @pl.loop(1, stages)
    def _(m):
        add(m)

    weights = pltpu.make_async_copy(weights_ref, w_ref, loads.at[1])
    weights.start()
    for r in range(n_rounds):
        pl.semaphore_wait(rounds.at[r], len(near))
        if r == n_rounds - 1:
            break
        if r == n_rounds - 2:
            @pl.when(outer == 1)
            def _():
                pl.semaphore_wait(met.at[0], cols - 1)
        near_signal(rounds.at[r + 1])
        for k in rest:
            if level[k] == r + 2:
                forward(0, pair(k)).start()
    for k in rest:
        if level[k] == n_rounds + 1 and n_rounds:
            forward(0, pair(k)).start()

    @pl.loop(1, stages)
    def _(m):
        for k in rest:
            forward(m, pair(k)).start()

    dot = functools.partial(jnp.dot, precision=HIGH, preferred_element_type=jnp.float32)

    @pl.loop(0, stages)
    def _(m):
        settle(x_ref.at[m, pl.ds(0, parts - 1)], frecv.at[m])
        x = x_ref[m].reshape(side, wide)
        g_ref[m * cols + t] = lax.dot_general(x, x, (((1,), (1,)), ((), ())), precision=HIGH, preferred_element_type=jnp.float32)
        for k in range(1, cols):
            partial(m, lax.rem(t + k, cols)).start()
        settle(g_ref.at[pl.ds(m * cols, cols - 1)], grecv.at[lax.rem(m, 2)])
        gram = g_ref[m * cols]
        for k in range(1, cols):
            gram = gram + g_ref[m * cols + k]
        total = polynomial(gram, dot, lambda a: jnp.sum(jnp.sum(a, axis=1, keepdims=True), axis=0, keepdims=True))
        y_ref[m] = dot(total, x_ref[m].reshape(side, wide)).reshape(parts, rows, wide)

        @pl.when(m < last)
        def _():
            for peer in outside[:-1] + inside:
                backward(m, peer, brecv.at[0]).start()

        @pl.when(m < last - 1)
        def _():
            backward(m, outside[-1], brecv.at[0]).start()

        @pl.when(m == last)
        def _():
            for peer in inside:
                backward(m, peer, blast.at[0]).start()
            backward(m, outside[0], blast.at[1 + f % half]).start()
            if last:
                backward(last - 1, outside[-1], brecv.at[0]).start()
            for peer in outside[1:-1]:
                backward(m, peer, blast.at[1 + f % half]).start()

            @pl.when(t % 2 == 0)
            def _():
                backward(m, outside[-1], blast.at[1 + f % half]).start()

    def finish(m, peers):
        for peer in peers:
            mat = m * parts + peer
            new_ref[mat] = w_ref[mat] - learn_rate * back_ref[mat]

    weights.wait()
    for m in range(stages):
        new_ref[m * parts + f] = w_ref[m * parts + f] - learn_rate * y_ref[m, f]
    if last:
        settle(back_ref.at[pl.ds(0, last * (parts - 1))], brecv.at[0])

        @pl.loop(0, last)
        def _(m):
            finish(m, inside + outside)

    @pl.when(t % 2 == 1)
    def _():
        settle(back_ref.at[pl.ds(0, mats - stages - 1)], bsend.at[0])
        backward(last, outside[-1], blast.at[1 + f % half]).start()

    if inside:
        settle(back_ref.at[pl.ds(0, len(inside))], blast.at[0])
        finish(last, inside)
    for peer in outside:
        settle(back_ref.at[last * parts + peer], blast.at[1 + peer % half])
        finish(last, [peer])

    settle(momentum_ref.at[pl.ds(0, mats - stages)], fsend.at[0])
    @pl.when(t % 2 == 1)
    def _():
        settle(back_ref.at[pl.ds(0, 1)], bsend.at[0])

    @pl.when(t % 2 == 0)
    def _():
        settle(back_ref.at[pl.ds(0, mats - stages)], bsend.at[0])

    settle(g_ref.at[pl.ds(0, stages * (cols - 1))], gsend.at[0])


def neighbours(parts):
    near = [k for k in (parts - 2, *(2**b for b in range(1, parts.bit_length() - 2)), 1) if k]
    near = list(dict.fromkeys(near))
    level, edge = {0: 0}, [0]
    while edge:
        found = {}
        for k in edge:
            for step in near:
                if k ^ step not in level:
                    found[k ^ step] = level[k] + 1
        level.update(found)
        edge = list(found)
    return near, level


def leave(first_ref, second_ref, first_out, second_out, sems):
    copies = [pltpu.make_async_copy(first_ref, first_out, sems.at[0]), pltpu.make_async_copy(second_ref, second_out, sems.at[1])]
    for copy in copies:
        copy.start()
    for copy in copies:
        copy.wait()


def leave_kernel(first, second):
    return pl.pallas_call(
        leave,
        out_shape=[jax.ShapeDtypeStruct(a.shape, a.dtype) for a in (first, second)],
        in_specs=[pl.BlockSpec(memory_space=pl.ANY)] * 2,
        out_specs=[pl.BlockSpec(memory_space=pl.ANY)] * 2,
        scratch_shapes=[pltpu.SemaphoreType.DMA((2,))],
        compiler_params=pltpu.CompilerParams(vmem_limit_bytes=2**20),
    )(first, second)


def iterate_kernel(slopes_in, moments_in, weights_in, parts, cols):
    mats, rows, wide = slopes_in.shape
    stages, side = mats // parts, rows * parts
    dma = pltpu.SemaphoreType.DMA
    n_rounds = max(1, max(neighbours(parts)[1].values()) - 1)
    return pl.pallas_call(
        functools.partial(kernel, stages, parts, cols),
        out_shape=[jax.ShapeDtypeStruct(slopes_in.shape, slopes_in.dtype)] * 2,
        in_specs=[pl.BlockSpec(memory_space=pltpu.HBM)] * 3,
        out_specs=[pl.BlockSpec(memory_space=pltpu.VMEM)] * 2,
        scratch_shapes=[
            pltpu.VMEM((2, stages, rows, wide), jnp.float32),
            pltpu.VMEM((2, mats, rows, wide), jnp.float32),
            *[pltpu.VMEM((mats, rows, wide), jnp.float32)] * 2,
            *[pltpu.VMEM((stages, parts, rows, wide), jnp.float32)] * 2,
            pltpu.VMEM((stages * cols, side, side), jnp.float32),
            dma((2,)), dma((1,)), dma((stages,)), dma((1,)), dma((1,)), dma((1 + parts // 2,)),
            dma((1,)), dma((2,)), pltpu.SemaphoreType.REGULAR((1,)), pltpu.SemaphoreType.REGULAR((n_rounds,)),
        ],
        compiler_params=pltpu.CompilerParams(collective_id=0, has_side_effects=True, vmem_limit_bytes=48 * 2**20),
    )(slopes_in, moments_in, weights_in)


def iterate_plain(new_momentum):
    moved = lax.all_to_all(new_momentum, "fsdp", split_axis=0, concat_axis=1, tiled=True)
    gram = lax.psum(jnp.einsum("mik,mjk->mij", moved, moved, precision=HIGH), "tp")
    dot = functools.partial(jnp.einsum, "mij,mjk->mik", precision=HIGH)
    total = polynomial(gram, dot, lambda a: jnp.sum(a, axis=(1, 2), keepdims=True))
    return lax.all_to_all(dot(total, moved), "fsdp", split_axis=1, concat_axis=0, tiled=True)


def body(parts, cols, slopes_in, moments_in, weights_in):
    if slopes_in.shape[1] % 8 == 0 and parts.bit_count() == 1 and parts // 2 > 2:
        new_momentum, new_weights = iterate_kernel(slopes_in, moments_in, weights_in, parts, cols)
        new_weights, new_momentum = leave_kernel(new_weights, new_momentum)
    else:
        new_momentum = hold_rate * moments_in + slopes_in
        new_weights = weights_in - learn_rate * iterate_plain(new_momentum)
    return (new_weights, new_momentum)


def solution(mesh):
    return jax.shard_map(
        functools.partial(body, mesh.shape["fsdp"], mesh.shape["tp"]),
        mesh=mesh,
        in_specs=(P(None, "fsdp", "tp"), P(None, "fsdp", "tp"), P(None, "fsdp", "tp")),
        out_specs=(P(None, "fsdp", "tp"), P(None, "fsdp", "tp")),
        check_vma=False,
    )
```

```python
import functools

import jax
import jax.numpy as jnp
from jax import lax
from jax.experimental import pallas as pl
from jax.experimental.pallas import tpu as pltpu
from jax.sharding import PartitionSpec as P

ITERS = 5
HIGH = lax.Precision.HIGHEST
MESH = pl.DeviceIdType.MESH


hold_rate = 0.8
learn_rate = 1.0


def polynomial(gram, dot, trace):
    side = gram.shape[-1]
    eye = jnp.where(
        lax.broadcasted_iota(jnp.int32, (side, side), 0) == lax.broadcasted_iota(jnp.int32, (side, side), 1), 1.0, 0.0
    ).astype(gram.dtype)
    scale = lax.rsqrt(trace(gram * eye) + 1e-06)
    gram = gram * (scale * scale)
    total = None
    for step in range(ITERS):
        mixed = 3.4445 * eye - 4.775 * gram + 2.0315 * dot(gram, gram)
        total = mixed * scale if total is None else dot(mixed, total)
        if step < ITERS - 1:
            gram = dot(dot(mixed, gram), mixed)
    return total


def kernel(
    stages, parts, cols, slopes_ref, moments_ref, weights_ref, momentum_ref, new_ref,
    first_ref, sm_ref, w_ref, back_ref, x_ref, y_ref, g_ref, loads, fsend, frecv, bsend, brecv, blast, gsend, grecv, met, rounds,
):
    rows, wide = momentum_ref.shape[1:]
    side, mats, half, last = parts * rows, stages * parts, parts // 2, stages - 1
    f, t = lax.axis_index("fsdp"), lax.axis_index("tp")
    upper = f // half

    def pair(k):
        peer = f
        for bit in range(k.bit_length()):
            if k >> bit & 1:
                peer = peer + (1 - 2 * ((f // 2**bit) % 2)) * 2**bit
        return peer

    middle = (f // 2 == half // 2 - 1) | (f // 2 == half // 2)
    outer = jnp.where(middle, 0, 1)
    first, ahead = parts - 2, first_ref.shape[1]
    known = [[], [half, half - 1, 2], [half + 1, 1], [parts - 1]]
    rest = [k for k in range(parts - 1, 0, -1) if k != first]
    inside = [pair(k) for k in range(half - 1, 0, -1)]
    outside = []
    for j in range(half // 2):
        z = upper * j + (1 - upper) * (half - 1 - j)
        x = f % 2 if j == half // 2 - 1 else 1
        outside += [2 * z + 1 - x, 2 * z + x]

    def greet(sem, *ks):
        for k in ks:
            pl.semaphore_signal(sem, inc=1, device_id={"fsdp": pair(k)}, device_id_type=MESH)

    def greet_tp(sem):
        for k in range(1, cols):
            pl.semaphore_signal(sem, inc=1, device_id={"tp": lax.rem(t + k, cols)}, device_id_type=MESH)

    barrier = pltpu.get_barrier_semaphore()

    def load_first(m, sem):
        mat = m * parts + pair(first)
        pltpu.make_async_copy(slopes_ref.at[mat], first_ref.at[0, m], sem).start()
        pltpu.make_async_copy(moments_ref.at[mat], first_ref.at[1, m], sem).start()

    load_first(0, loads.at[0])
    greet(barrier, first)

    @pl.when(middle)
    def _():
        greet(barrier, 2)

    for m in range(1, ahead):
        load_first(m, loads.at[1])

    @pl.when(outer == 1)
    def _():
        greet(barrier, 1)
        greet_tp(barrier)

    def forward(m, peer):
        return pltpu.make_async_remote_copy(
            src_ref=momentum_ref.at[m * parts + peer], dst_ref=x_ref.at[m, f],
            send_sem=fsend.at[0], recv_sem=frecv.at[m],
            device_id={"fsdp": peer}, device_id_type=MESH,
        )

    def backward(m, peer, recv):
        return pltpu.make_async_remote_copy(
            src_ref=y_ref.at[m, peer], dst_ref=back_ref.at[m * parts + f],
            send_sem=bsend.at[0], recv_sem=recv,
            device_id={"fsdp": peer}, device_id_type=MESH,
        )

    def partial(m, peer):
        return pltpu.make_async_remote_copy(
            src_ref=g_ref.at[m * cols + t], dst_ref=g_ref.at[m * cols + t],
            send_sem=gsend.at[0], recv_sem=grecv.at[lax.rem(m, 2)],
            device_id={"tp": peer}, device_id_type=MESH,
        )

    def settle(ref, sem):
        pltpu.make_async_copy(ref, ref, sem).wait()

    def add(m):
        for k in [0, *rest]:
            mat = m * parts + pair(k)
            value = hold_rate * sm_ref[1, mat] + sm_ref[0, mat]
            momentum_ref[mat] = value
            if k == 0:
                x_ref[m, f] = value

        @pl.when(m >= ahead)
        def _():
            mat = m * parts + pair(first)
            momentum_ref[mat] = hold_rate * sm_ref[1, mat] + sm_ref[0, mat]

    settle(first_ref.at[:, 0], loads.at[0])
    momentum_ref[pair(first)] = hold_rate * first_ref[1, 0] + first_ref[0, 0]
    for which, src in enumerate((slopes_ref, moments_ref)):
        pltpu.make_async_copy(src, sm_ref.at[which], loads.at[0]).start()
    pl.semaphore_wait(barrier, 1 + outer * (cols + 1))
    forward(0, pair(first)).start()
    if ahead > 1:
        settle(first_ref.at[:, pl.ds(1, ahead - 1)], loads.at[1])
    for m in range(1, ahead):
        momentum_ref[m * parts + pair(first)] = hold_rate * first_ref[1, m] + first_ref[0, m]
        forward(m, pair(first)).start()

    @pl.when(outer == 1)
    def _():
        greet(rounds.at[0], 2, 1, first)
        greet_tp(met.at[0])

    settle(sm_ref, loads.at[0])

    @pl.loop(0, stages)
    def _(m):
        add(m)

    weights = pltpu.make_async_copy(weights_ref, w_ref, loads.at[1])
    weights.start()

    pl.semaphore_wait(rounds.at[0], 1 + outer)

    @pl.when(outer == 1)
    def _():
        pl.semaphore_wait(met.at[0], cols - 1)
        greet(rounds.at[1], 2, 1, first)

    for k in known[1]:
        forward(0, pair(k)).start()
    pl.semaphore_wait(rounds.at[1], 1 + outer)

    @pl.when(outer == 1)
    def _():
        greet(rounds.at[2], 2)

    for k in known[2]:
        forward(0, pair(k)).start()

    @pl.when(middle)
    def _():
        pl.semaphore_wait(rounds.at[2], 1)

    for k in known[3]:
        forward(0, pair(k)).start()

    @pl.loop(1, stages)
    def _(m):
        for k in rest:
            forward(m, pair(k)).start()

        @pl.when(m >= ahead)
        def _():
            forward(m, pair(first)).start()

    dot = functools.partial(jnp.dot, precision=HIGH, preferred_element_type=jnp.float32)

    @pl.loop(0, stages)
    def _(m):
        settle(x_ref.at[m, pl.ds(0, parts - 1)], frecv.at[m])
        x = x_ref[m].reshape(side, wide)
        g_ref[m * cols + t] = lax.dot_general(x, x, (((1,), (1,)), ((), ())), precision=HIGH, preferred_element_type=jnp.float32)
        for k in range(1, cols):
            partial(m, lax.rem(t + k, cols)).start()
        settle(g_ref.at[pl.ds(m * cols, cols - 1)], grecv.at[lax.rem(m, 2)])
        gram = g_ref[m * cols]
        for k in range(1, cols):
            gram = gram + g_ref[m * cols + k]
        total = polynomial(gram, dot, lambda a: jnp.sum(jnp.sum(a, axis=1, keepdims=True), axis=0, keepdims=True))
        y_ref[m] = dot(total, x_ref[m].reshape(side, wide)).reshape(parts, rows, wide)

        @pl.when(m < last)
        def _():
            for peer in outside[:-1] + inside:
                backward(m, peer, brecv.at[0]).start()

        @pl.when(m < last - 1)
        def _():
            backward(m, outside[-1], brecv.at[0]).start()

        @pl.when(m == last)
        def _():
            for peer in inside:
                backward(m, peer, blast.at[0]).start()
            backward(m, outside[0], blast.at[1 + f % half]).start()
            if last:
                backward(last - 1, outside[-1], brecv.at[0]).start()
            for peer in outside[1:-1]:
                backward(m, peer, blast.at[1 + f % half]).start()

            @pl.when(t % 2 == 0)
            def _():
                backward(m, outside[-1], blast.at[1 + f % half]).start()

    def finish(m, peers):
        for peer in peers:
            mat = m * parts + peer
            new_ref[mat] = w_ref[mat] - learn_rate * back_ref[mat]

    weights.wait()
    for m in range(stages):
        new_ref[m * parts + f] = w_ref[m * parts + f] - learn_rate * y_ref[m, f]
    if last:
        settle(back_ref.at[pl.ds(0, last * (parts - 1))], brecv.at[0])

        @pl.loop(0, last)
        def _(m):
            finish(m, inside + outside)

    @pl.when(t % 2 == 1)
    def _():
        settle(back_ref.at[pl.ds(0, mats - stages - 1)], bsend.at[0])
        backward(last, outside[-1], blast.at[1 + f % half]).start()

    if inside:
        settle(back_ref.at[pl.ds(0, len(inside))], blast.at[0])
        finish(last, inside)
    for peer in outside:
        settle(back_ref.at[last * parts + peer], blast.at[1 + peer % half])
        finish(last, [peer])

    settle(momentum_ref.at[pl.ds(0, mats - stages)], fsend.at[0])
    @pl.when(t % 2 == 1)
    def _():
        settle(back_ref.at[pl.ds(0, 1)], bsend.at[0])

    @pl.when(t % 2 == 0)
    def _():
        settle(back_ref.at[pl.ds(0, mats - stages)], bsend.at[0])

    settle(g_ref.at[pl.ds(0, stages * (cols - 1))], gsend.at[0])


def leave(first_ref, second_ref, first_out, second_out, sems):
    copies = [pltpu.make_async_copy(first_ref, first_out, sems.at[0]), pltpu.make_async_copy(second_ref, second_out, sems.at[1])]
    for copy in copies:
        copy.start()
    for copy in copies:
        copy.wait()


def leave_kernel(first, second):
    return pl.pallas_call(
        leave,
        out_shape=[jax.ShapeDtypeStruct(a.shape, a.dtype) for a in (first, second)],
        in_specs=[pl.BlockSpec(memory_space=pl.ANY)] * 2,
        out_specs=[pl.BlockSpec(memory_space=pl.ANY)] * 2,
        scratch_shapes=[pltpu.SemaphoreType.DMA((2,))],
        compiler_params=pltpu.CompilerParams(vmem_limit_bytes=2**20),
    )(first, second)


def iterate_kernel(slopes_in, moments_in, weights_in, parts, cols):
    mats, rows, wide = slopes_in.shape
    stages, side = mats // parts, rows * parts
    dma = pltpu.SemaphoreType.DMA
    ahead = (stages + 1) // 2
    return pl.pallas_call(
        functools.partial(kernel, stages, parts, cols),
        out_shape=[jax.ShapeDtypeStruct(slopes_in.shape, slopes_in.dtype)] * 2,
        in_specs=[pl.BlockSpec(memory_space=pltpu.HBM)] * 3,
        out_specs=[pl.BlockSpec(memory_space=pltpu.VMEM)] * 2,
        scratch_shapes=[
            pltpu.VMEM((2, ahead, rows, wide), jnp.float32),
            pltpu.VMEM((2, mats, rows, wide), jnp.float32),
            *[pltpu.VMEM((mats, rows, wide), jnp.float32)] * 2,
            *[pltpu.VMEM((stages, parts, rows, wide), jnp.float32)] * 2,
            pltpu.VMEM((stages * cols, side, side), jnp.float32),
            dma((2,)), dma((1,)), dma((stages,)), dma((1,)), dma((1,)), dma((1 + parts // 2,)),
            dma((1,)), dma((2,)), pltpu.SemaphoreType.REGULAR((1,)), pltpu.SemaphoreType.REGULAR((3,)),
        ],
        compiler_params=pltpu.CompilerParams(collective_id=0, has_side_effects=True, vmem_limit_bytes=48 * 2**20),
    )(slopes_in, moments_in, weights_in)


def iterate_plain(new_momentum):
    moved = lax.all_to_all(new_momentum, "fsdp", split_axis=0, concat_axis=1, tiled=True)
    gram = lax.psum(jnp.einsum("mik,mjk->mij", moved, moved, precision=HIGH), "tp")
    dot = functools.partial(jnp.einsum, "mij,mjk->mik", precision=HIGH)
    total = polynomial(gram, dot, lambda a: jnp.sum(a, axis=(1, 2), keepdims=True))
    return lax.all_to_all(dot(total, moved), "fsdp", split_axis=1, concat_axis=0, tiled=True)


def body(parts, cols, slopes_in, moments_in, weights_in):
    if slopes_in.shape[1] % 8 == 0 and parts // 4 == 2 and parts % 4 == 0:
        new_momentum, new_weights = iterate_kernel(slopes_in, moments_in, weights_in, parts, cols)
        new_weights, new_momentum = leave_kernel(new_weights, new_momentum)
    else:
        new_momentum = hold_rate * moments_in + slopes_in
        new_weights = weights_in - learn_rate * iterate_plain(new_momentum)
    return (new_weights, new_momentum)


def solution(mesh):
    return jax.shard_map(
        functools.partial(body, mesh.shape["fsdp"], mesh.shape["tp"]),
        mesh=mesh,
        in_specs=(P(None, "fsdp", "tp"), P(None, "fsdp", "tp"), P(None, "fsdp", "tp")),
        out_specs=(P(None, "fsdp", "tp"), P(None, "fsdp", "tp")),
        check_vma=False,
    )
```

```python
import functools

import jax
import jax.numpy as jnp
from jax import lax
from jax.experimental import pallas as pl
from jax.experimental.pallas import tpu as pltpu
from jax.sharding import PartitionSpec as P

ITERS = 5
HIGH = lax.Precision.HIGHEST
MESH = pl.DeviceIdType.MESH


hold_rate = 0.8
learn_rate = 1.0


def polynomial(gram, dot, trace):
    side = gram.shape[-1]
    eye = jnp.where(
        lax.broadcasted_iota(jnp.int32, (side, side), 0) == lax.broadcasted_iota(jnp.int32, (side, side), 1), 1.0, 0.0
    ).astype(gram.dtype)
    scale = lax.rsqrt(trace(gram * eye) + 1e-06)
    gram = gram * (scale * scale)
    total = None
    for step in range(ITERS):
        mixed = 3.4445 * eye - 4.775 * gram + 2.0315 * dot(gram, gram)
        total = mixed * scale if total is None else dot(mixed, total)
        if step < ITERS - 1:
            gram = dot(dot(mixed, gram), mixed)
    return total


def kernel(
    stages, parts, cols, slopes_ref, moments_ref, weights_ref, momentum_ref, new_ref,
    first_ref, sm_ref, w_ref, back_ref, x_ref, y_ref, g_ref, loads, fsend, frecv, bsend, brecv, blast, gsend, grecv, met, rounds,
):
    rows, wide = momentum_ref.shape[1:]
    side, mats, half, last = parts * rows, stages * parts, parts // 2, stages - 1
    f, t = lax.axis_index("fsdp"), lax.axis_index("tp")
    upper = f // half
    soon, late = (slice(None), pl.ds(0, wide // 4)), (slice(None), pl.ds(wide // 4, wide - wide // 4))

    def pair(k):
        peer = f
        for bit in range(k.bit_length()):
            if k >> bit & 1:
                peer = peer + (1 - 2 * ((f // 2**bit) % 2)) * 2**bit
        return peer

    middle = (f // 2 == half // 2 - 1) | (f // 2 == half // 2)
    outer = jnp.where(middle, 0, 1)
    first, ahead = parts - 2, first_ref.shape[1]
    known = [[], [half, half - 1, 2], [half + 1, 1], [parts - 1]]
    rest = [k for k in range(parts - 1, 0, -1) if k != first]
    inside = [pair(k) for k in range(half - 1, 0, -1)]
    outside = []
    for j in range(half // 2):
        z = upper * j + (1 - upper) * (half - 1 - j)
        x = f % 2 if j == half // 2 - 1 else 1
        outside += [2 * z + 1 - x, 2 * z + x]

    def greet(sem, *ks):
        for k in ks:
            pl.semaphore_signal(sem, inc=1, device_id={"fsdp": pair(k)}, device_id_type=MESH)

    def greet_tp(sem):
        for k in range(1, cols):
            pl.semaphore_signal(sem, inc=1, device_id={"tp": lax.rem(t + k, cols)}, device_id_type=MESH)

    barrier = pltpu.get_barrier_semaphore()

    def load_first(m, sem):
        mat = m * parts + pair(first)
        for piece in range(2):
            part = pl.ds(piece * rows // 2, rows // 2)
            pltpu.make_async_copy(slopes_ref.at[mat, part], first_ref.at[0, m, part], sem).start()
            pltpu.make_async_copy(moments_ref.at[mat, part], first_ref.at[1, m, part], sem).start()

    load_first(0, loads.at[0])
    greet(barrier, first)

    @pl.when(middle)
    def _():
        greet(barrier, 2)

    for m in range(1, ahead):
        load_first(m, loads.at[1])

    @pl.when(outer == 1)
    def _():
        greet(barrier, 1)
        greet_tp(barrier)

    def forward(m, peer):
        return pltpu.make_async_remote_copy(
            src_ref=momentum_ref.at[m * parts + peer], dst_ref=x_ref.at[m, f],
            send_sem=fsend.at[0], recv_sem=frecv.at[m],
            device_id={"fsdp": peer}, device_id_type=MESH,
        )

    def backward(m, peer, recv, *part):
        return pltpu.make_async_remote_copy(
            src_ref=y_ref.at[m, peer, *part], dst_ref=back_ref.at[m * parts + f, *part],
            send_sem=bsend.at[0], recv_sem=recv,
            device_id={"fsdp": peer}, device_id_type=MESH,
        )

    def partial(m, peer):
        return pltpu.make_async_remote_copy(
            src_ref=g_ref.at[m * cols + t], dst_ref=g_ref.at[m * cols + t],
            send_sem=gsend.at[0], recv_sem=grecv.at[lax.rem(m, 2)],
            device_id={"tp": peer}, device_id_type=MESH,
        )

    def settle(ref, sem):
        pltpu.make_async_copy(ref, ref, sem).wait()

    def add(m):
        for k in [0, *rest]:
            mat = m * parts + pair(k)
            value = hold_rate * sm_ref[1, mat] + sm_ref[0, mat]
            momentum_ref[mat] = value
            if k == 0:
                x_ref[m, f] = value

        @pl.when(m >= ahead)
        def _():
            mat = m * parts + pair(first)
            momentum_ref[mat] = hold_rate * sm_ref[1, mat] + sm_ref[0, mat]

    settle(first_ref.at[:, 0], loads.at[0])
    momentum_ref[pair(first)] = hold_rate * first_ref[1, 0] + first_ref[0, 0]
    for which, src in enumerate((slopes_ref, moments_ref)):
        pltpu.make_async_copy(src, sm_ref.at[which], loads.at[0]).start()
    pl.semaphore_wait(barrier, 1 + outer * (cols + 1))
    forward(0, pair(first)).start()
    if ahead > 1:
        settle(first_ref.at[:, pl.ds(1, ahead - 1)], loads.at[1])
    for m in range(1, ahead):
        momentum_ref[m * parts + pair(first)] = hold_rate * first_ref[1, m] + first_ref[0, m]
        forward(m, pair(first)).start()

    @pl.when(outer == 1)
    def _():
        greet(rounds.at[0], 2, 1, first)
        greet_tp(met.at[0])

    settle(sm_ref, loads.at[0])

    @pl.loop(0, stages)
    def _(m):
        add(m)

    weights = pltpu.make_async_copy(weights_ref, w_ref, loads.at[1])
    weights.start()

    pl.semaphore_wait(rounds.at[0], 1 + outer)

    @pl.when(outer == 1)
    def _():
        pl.semaphore_wait(met.at[0], cols - 1)
        greet(rounds.at[1], 2, 1, first)

    for k in known[1]:
        forward(0, pair(k)).start()
    pl.semaphore_wait(rounds.at[1], 1 + outer)

    @pl.when(outer == 1)
    def _():
        greet(rounds.at[2], 2)

    for k in known[2]:
        forward(0, pair(k)).start()

    @pl.when(middle)
    def _():
        pl.semaphore_wait(rounds.at[2], 1)

    for k in known[3]:
        forward(0, pair(k)).start()

    @pl.loop(1, stages)
    def _(m):
        for k in rest:
            forward(m, pair(k)).start()

        @pl.when(m >= ahead)
        def _():
            forward(m, pair(first)).start()

    dot = functools.partial(jnp.dot, precision=HIGH, preferred_element_type=jnp.float32)

    @pl.loop(0, stages)
    def _(m):
        settle(x_ref.at[m, pl.ds(0, parts - 1)], frecv.at[m])
        x = x_ref[m].reshape(side, wide)
        g_ref[m * cols + t] = lax.dot_general(x, x, (((1,), (1,)), ((), ())), precision=HIGH, preferred_element_type=jnp.float32)
        for k in range(1, cols):
            partial(m, lax.rem(t + k, cols)).start()
        settle(g_ref.at[pl.ds(m * cols, cols - 1)], grecv.at[lax.rem(m, 2)])
        gram = g_ref[m * cols]
        for k in range(1, cols):
            gram = gram + g_ref[m * cols + k]
        total = polynomial(gram, dot, lambda a: jnp.sum(jnp.sum(a, axis=1, keepdims=True), axis=0, keepdims=True))
        y_ref[m] = dot(total, x_ref[m].reshape(side, wide)).reshape(parts, rows, wide)

        @pl.when(m < last)
        def _():
            for peer in outside[:-1] + inside:
                backward(m, peer, brecv.at[0]).start()

        @pl.when(m < last - 1)
        def _():
            backward(m, outside[-1], brecv.at[0]).start()

        @pl.when(m == last)
        def _():
            for peer in inside:
                backward(m, peer, blast.at[0]).start()
            backward(m, outside[0], blast.at[1 + f % half]).start()
            if last:
                backward(last - 1, outside[-1], brecv.at[0]).start()
            for peer in outside[1:-1]:
                backward(m, peer, blast.at[1 + f % half]).start()

            backward(m, outside[-1], blast.at[1 + f % half], *soon).start()

            @pl.when(t % 2 == 0)
            def _():
                backward(m, outside[-1], blast.at[1 + f % half], *late).start()

    def finish(m, peers):
        for peer in peers:
            mat = m * parts + peer
            new_ref[mat] = w_ref[mat] - learn_rate * back_ref[mat]

    weights.wait()
    for m in range(stages):
        new_ref[m * parts + f] = w_ref[m * parts + f] - learn_rate * y_ref[m, f]
    if last:
        settle(back_ref.at[pl.ds(0, last * (parts - 1))], brecv.at[0])

        @pl.loop(0, last)
        def _(m):
            finish(m, inside + outside)

    @pl.when(t % 2 == 1)
    def _():
        settle(back_ref.at[pl.ds(0, mats - stages - 1)], bsend.at[0])
        backward(last, outside[-1], blast.at[1 + f % half], *late).start()

    if inside:
        settle(back_ref.at[pl.ds(0, len(inside))], blast.at[0])
        finish(last, inside)
    for peer in outside:
        settle(back_ref.at[last * parts + peer], blast.at[1 + peer % half])
        finish(last, [peer])

    settle(momentum_ref.at[pl.ds(0, mats - stages)], fsend.at[0])
    @pl.when(t % 2 == 1)
    def _():
        settle(back_ref.at[pl.ds(0, 1)], bsend.at[0])

    @pl.when(t % 2 == 0)
    def _():
        settle(back_ref.at[pl.ds(0, mats - stages)], bsend.at[0])

    settle(g_ref.at[pl.ds(0, stages * (cols - 1))], gsend.at[0])


def leave(first_ref, second_ref, first_out, second_out, sems):
    copies = [pltpu.make_async_copy(first_ref, first_out, sems.at[0]), pltpu.make_async_copy(second_ref, second_out, sems.at[1])]
    for copy in copies:
        copy.start()
    for copy in copies:
        copy.wait()


def leave_kernel(first, second):
    return pl.pallas_call(
        leave,
        out_shape=[jax.ShapeDtypeStruct(a.shape, a.dtype) for a in (first, second)],
        in_specs=[pl.BlockSpec(memory_space=pl.ANY)] * 2,
        out_specs=[pl.BlockSpec(memory_space=pl.ANY)] * 2,
        scratch_shapes=[pltpu.SemaphoreType.DMA((2,))],
        compiler_params=pltpu.CompilerParams(vmem_limit_bytes=2**20),
    )(first, second)


def iterate_kernel(slopes_in, moments_in, weights_in, parts, cols):
    mats, rows, wide = slopes_in.shape
    stages, side = mats // parts, rows * parts
    dma = pltpu.SemaphoreType.DMA
    ahead = (stages + 1) // 2
    return pl.pallas_call(
        functools.partial(kernel, stages, parts, cols),
        out_shape=[jax.ShapeDtypeStruct(slopes_in.shape, slopes_in.dtype)] * 2,
        in_specs=[pl.BlockSpec(memory_space=pltpu.HBM)] * 3,
        out_specs=[pl.BlockSpec(memory_space=pltpu.VMEM)] * 2,
        scratch_shapes=[
            pltpu.VMEM((2, ahead, rows, wide), jnp.float32),
            pltpu.VMEM((2, mats, rows, wide), jnp.float32),
            *[pltpu.VMEM((mats, rows, wide), jnp.float32)] * 2,
            *[pltpu.VMEM((stages, parts, rows, wide), jnp.float32)] * 2,
            pltpu.VMEM((stages * cols, side, side), jnp.float32),
            dma((2,)), dma((1,)), dma((stages,)), dma((1,)), dma((1,)), dma((1 + parts // 2,)),
            dma((1,)), dma((2,)), pltpu.SemaphoreType.REGULAR((1,)), pltpu.SemaphoreType.REGULAR((3,)),
        ],
        compiler_params=pltpu.CompilerParams(collective_id=0, has_side_effects=True, vmem_limit_bytes=48 * 2**20),
    )(slopes_in, moments_in, weights_in)


def iterate_plain(new_momentum):
    moved = lax.all_to_all(new_momentum, "fsdp", split_axis=0, concat_axis=1, tiled=True)
    gram = lax.psum(jnp.einsum("mik,mjk->mij", moved, moved, precision=HIGH), "tp")
    dot = functools.partial(jnp.einsum, "mij,mjk->mik", precision=HIGH)
    total = polynomial(gram, dot, lambda a: jnp.sum(a, axis=(1, 2), keepdims=True))
    return lax.all_to_all(dot(total, moved), "fsdp", split_axis=1, concat_axis=0, tiled=True)


def body(parts, cols, slopes_in, moments_in, weights_in):
    if slopes_in.shape[1] % 8 == 0 and parts // 4 == 2 and parts % 4 == 0:
        new_momentum, new_weights = iterate_kernel(slopes_in, moments_in, weights_in, parts, cols)
        new_weights, new_momentum = leave_kernel(new_weights, new_momentum)
    else:
        new_momentum = hold_rate * moments_in + slopes_in
        new_weights = weights_in - learn_rate * iterate_plain(new_momentum)
    return (new_weights, new_momentum)


def solution(mesh):
    return jax.shard_map(
        functools.partial(body, mesh.shape["fsdp"], mesh.shape["tp"]),
        mesh=mesh,
        in_specs=(P(None, "fsdp", "tp"), P(None, "fsdp", "tp"), P(None, "fsdp", "tp")),
        out_specs=(P(None, "fsdp", "tp"), P(None, "fsdp", "tp")),
        check_vma=False,
    )
```

```python
import functools

import jax
import jax.numpy as jnp
from jax import lax
from jax.experimental import pallas as pl
from jax.experimental.pallas import tpu as pltpu
from jax.sharding import PartitionSpec as P

ITERS = 5
HIGH = lax.Precision.HIGHEST
MESH = pl.DeviceIdType.MESH


hold_rate = 0.8
learn_rate = 1.0


def polynomial(gram, dot, trace):
    side = gram.shape[-1]
    eye = jnp.where(
        lax.broadcasted_iota(jnp.int32, (side, side), 0) == lax.broadcasted_iota(jnp.int32, (side, side), 1), 1.0, 0.0
    ).astype(gram.dtype)
    scale = lax.rsqrt(trace(gram * eye) + 1e-06)
    gram = gram * (scale * scale)
    total = None
    for step in range(ITERS):
        mixed = 3.4445 * eye - 4.775 * gram + 2.0315 * dot(gram, gram)
        total = mixed * scale if total is None else dot(mixed, total)
        if step < ITERS - 1:
            gram = dot(dot(mixed, gram), mixed)
    return total


def kernel(
    stages, parts, cols, slopes_ref, moments_ref, weights_ref, momentum_ref, new_ref,
    first_ref, sm_ref, w_ref, back_ref, x_ref, y_ref, g_ref, loads, fsend, frecv, bsend, brecv, blast, gsend, grecv, met, rounds,
):
    rows, wide = momentum_ref.shape[1:]
    side, mats, half, last = parts * rows, stages * parts, parts // 2, stages - 1
    f, t = lax.axis_index("fsdp"), lax.axis_index("tp")
    upper = f // half
    soon, late = (slice(None), pl.ds(0, wide // 4)), (slice(None), pl.ds(wide // 4, wide - wide // 4))

    def pair(k):
        peer = f
        for bit in range(k.bit_length()):
            if k >> bit & 1:
                peer = peer + (1 - 2 * ((f // 2**bit) % 2)) * 2**bit
        return peer

    middle = (f // 2 == half // 2 - 1) | (f // 2 == half // 2)
    outer = jnp.where(middle, 0, 1)
    first, ahead = parts - 2, first_ref.shape[1]
    known = [[], [half, half - 1, 2], [half + 1, 1], [parts - 1]]
    rest = [k for k in range(parts - 1, 0, -1) if k != first]
    inside = [pair(k) for k in range(half - 1, 0, -1)]
    outside = []
    for j in range(half // 2):
        z = upper * j + (1 - upper) * (half - 1 - j)
        x = f % 2 if j == half // 2 - 1 else 1
        outside += [2 * z + 1 - x, 2 * z + x]

    def greet(sem, *ks):
        for k in ks:
            pl.semaphore_signal(sem, inc=1, device_id={"fsdp": pair(k)}, device_id_type=MESH)

    def greet_tp(sem):
        for k in range(1, cols):
            pl.semaphore_signal(sem, inc=1, device_id={"tp": lax.rem(t + k, cols)}, device_id_type=MESH)

    barrier = pltpu.get_barrier_semaphore()

    def load_first(m, sem):
        mat = m * parts + pair(first)
        for piece in range(2):
            part = pl.ds(piece * rows // 2, rows // 2)
            pltpu.make_async_copy(slopes_ref.at[mat, part], first_ref.at[0, m, part], sem).start()
            pltpu.make_async_copy(moments_ref.at[mat, part], first_ref.at[1, m, part], sem).start()

    load_first(0, loads.at[0])
    greet(barrier, first)

    @pl.when(middle)
    def _():
        greet(barrier, 2)

    for m in range(1, ahead):
        load_first(m, loads.at[1])

    @pl.when(outer == 1)
    def _():
        greet(barrier, 1)
        greet_tp(barrier)

    def forward(m, peer):
        return pltpu.make_async_remote_copy(
            src_ref=momentum_ref.at[m * parts + peer], dst_ref=x_ref.at[m, f],
            send_sem=fsend.at[0], recv_sem=frecv.at[m],
            device_id={"fsdp": peer}, device_id_type=MESH,
        )

    def backward(m, peer, recv, *part):
        return pltpu.make_async_remote_copy(
            src_ref=y_ref.at[m, peer, *part], dst_ref=back_ref.at[m * parts + f, *part],
            send_sem=bsend.at[0], recv_sem=recv,
            device_id={"fsdp": peer}, device_id_type=MESH,
        )

    def partial(m, peer):
        return pltpu.make_async_remote_copy(
            src_ref=g_ref.at[m * cols + t], dst_ref=g_ref.at[m * cols + t],
            send_sem=gsend.at[0], recv_sem=grecv.at[lax.rem(m, 2)],
            device_id={"tp": peer}, device_id_type=MESH,
        )

    def settle(ref, sem):
        pltpu.make_async_copy(ref, ref, sem).wait()

    def add(m):
        for k in [0, *rest]:
            mat = m * parts + pair(k)
            value = hold_rate * sm_ref[1, mat] + sm_ref[0, mat]
            momentum_ref[mat] = value
            if k == 0:
                x_ref[m, f] = value

        @pl.when(m >= ahead)
        def _():
            mat = m * parts + pair(first)
            momentum_ref[mat] = hold_rate * sm_ref[1, mat] + sm_ref[0, mat]

    settle(first_ref.at[:, 0], loads.at[0])
    momentum_ref[pair(first)] = hold_rate * first_ref[1, 0] + first_ref[0, 0]
    for which, src in enumerate((slopes_ref, moments_ref)):
        pltpu.make_async_copy(src, sm_ref.at[which], loads.at[0]).start()
    pl.semaphore_wait(barrier, 1 + outer * (cols + 1))
    forward(0, pair(first)).start()
    if ahead > 1:
        settle(first_ref.at[:, pl.ds(1, ahead - 1)], loads.at[1])
    for m in range(1, ahead):
        momentum_ref[m * parts + pair(first)] = hold_rate * first_ref[1, m] + first_ref[0, m]
        forward(m, pair(first)).start()

    @pl.when(outer == 1)
    def _():
        greet(rounds.at[0], 2, 1, first)
        greet_tp(met.at[0])

    settle(sm_ref, loads.at[0])

    @pl.loop(0, stages)
    def _(m):
        add(m)

    weights = pltpu.make_async_copy(weights_ref, w_ref, loads.at[1])
    weights.start()

    pl.semaphore_wait(rounds.at[0], 1 + outer)

    @pl.when(outer == 1)
    def _():
        pl.semaphore_wait(met.at[0], cols - 1)
        greet(rounds.at[1], 2, 1, first)

    for k in known[1]:
        forward(0, pair(k)).start()
    pl.semaphore_wait(rounds.at[1], 1 + outer)

    @pl.when(outer == 1)
    def _():
        greet(rounds.at[2], 2)

    for k in known[2]:
        forward(0, pair(k)).start()

    @pl.when(middle)
    def _():
        pl.semaphore_wait(rounds.at[2], 1)

    for k in known[3]:
        forward(0, pair(k)).start()

    @pl.loop(1, stages)
    def _(m):
        for k in rest:
            forward(m, pair(k)).start()

        @pl.when(m >= ahead)
        def _():
            forward(m, pair(first)).start()

    dot = functools.partial(jnp.dot, precision=HIGH, preferred_element_type=jnp.float32)

    @pl.loop(0, stages)
    def _(m):
        settle(x_ref.at[m, pl.ds(0, parts - 1)], frecv.at[m])
        x = x_ref[m].reshape(side, wide)
        g_ref[m * cols + t] = lax.dot_general(x, x, (((1,), (1,)), ((), ())), precision=HIGH, preferred_element_type=jnp.float32)
        for k in range(1, cols):
            partial(m, lax.rem(t + k, cols)).start()
        settle(g_ref.at[pl.ds(m * cols, cols - 1)], grecv.at[lax.rem(m, 2)])
        gram = g_ref[m * cols]
        for k in range(1, cols):
            gram = gram + g_ref[m * cols + k]
        total = polynomial(gram, dot, lambda a: jnp.sum(jnp.sum(a, axis=1, keepdims=True), axis=0, keepdims=True))
        y_ref[m] = dot(total, x_ref[m].reshape(side, wide)).reshape(parts, rows, wide)

        @pl.when(m < last)
        def _():
            for peer in outside[:-1] + inside:
                backward(m, peer, brecv.at[0]).start()

        @pl.when(m < last - 1)
        def _():
            backward(m, outside[-1], brecv.at[0]).start()

        @pl.when(m == last)
        def _():
            for peer in inside:
                backward(m, peer, blast.at[0]).start()
            backward(m, outside[0], blast.at[1 + f % half]).start()
            for peer in outside[1:-1]:
                backward(m, peer, blast.at[1 + f % half]).start()
            if last:
                backward(last - 1, outside[-1], brecv.at[0]).start()

            backward(m, outside[-1], blast.at[1 + f % half], *soon).start()

            @pl.when(t % 2 == 0)
            def _():
                backward(m, outside[-1], blast.at[1 + f % half], *late).start()

    def finish(m, peers):
        for peer in peers:
            mat = m * parts + peer
            new_ref[mat] = w_ref[mat] - learn_rate * back_ref[mat]

    weights.wait()
    for m in range(stages):
        new_ref[m * parts + f] = w_ref[m * parts + f] - learn_rate * y_ref[m, f]
    @pl.when(t % 2 == 1)
    def _():
        settle(back_ref.at[pl.ds(0, mats - stages - 1)], bsend.at[0])
        backward(last, outside[-1], blast.at[1 + f % half], *late).start()

    if last:
        settle(back_ref.at[pl.ds(0, last * (parts - 1))], brecv.at[0])

        @pl.loop(0, last)
        def _(m):
            finish(m, inside + outside)

    if inside:
        settle(back_ref.at[pl.ds(0, len(inside))], blast.at[0])
        finish(last, inside)
    for peer in outside:
        settle(back_ref.at[last * parts + peer], blast.at[1 + peer % half])
        finish(last, [peer])

    settle(momentum_ref.at[pl.ds(0, mats - stages)], fsend.at[0])
    @pl.when(t % 2 == 1)
    def _():
        settle(back_ref.at[pl.ds(0, 1)], bsend.at[0])

    @pl.when(t % 2 == 0)
    def _():
        settle(back_ref.at[pl.ds(0, mats - stages)], bsend.at[0])

    settle(g_ref.at[pl.ds(0, stages * (cols - 1))], gsend.at[0])


def leave(first_ref, second_ref, first_out, second_out, sems):
    copies = [pltpu.make_async_copy(first_ref, first_out, sems.at[0]), pltpu.make_async_copy(second_ref, second_out, sems.at[1])]
    for copy in copies:
        copy.start()
    for copy in copies:
        copy.wait()


def leave_kernel(first, second):
    return pl.pallas_call(
        leave,
        out_shape=[jax.ShapeDtypeStruct(a.shape, a.dtype) for a in (first, second)],
        in_specs=[pl.BlockSpec(memory_space=pl.ANY)] * 2,
        out_specs=[pl.BlockSpec(memory_space=pl.ANY)] * 2,
        scratch_shapes=[pltpu.SemaphoreType.DMA((2,))],
        compiler_params=pltpu.CompilerParams(vmem_limit_bytes=2**20),
    )(first, second)


def iterate_kernel(slopes_in, moments_in, weights_in, parts, cols):
    mats, rows, wide = slopes_in.shape
    stages, side = mats // parts, rows * parts
    dma = pltpu.SemaphoreType.DMA
    ahead = (stages + 1) // 2
    return pl.pallas_call(
        functools.partial(kernel, stages, parts, cols),
        out_shape=[jax.ShapeDtypeStruct(slopes_in.shape, slopes_in.dtype)] * 2,
        in_specs=[pl.BlockSpec(memory_space=pltpu.HBM)] * 3,
        out_specs=[pl.BlockSpec(memory_space=pltpu.VMEM)] * 2,
        scratch_shapes=[
            pltpu.VMEM((2, ahead, rows, wide), jnp.float32),
            pltpu.VMEM((2, mats, rows, wide), jnp.float32),
            *[pltpu.VMEM((mats, rows, wide), jnp.float32)] * 2,
            *[pltpu.VMEM((stages, parts, rows, wide), jnp.float32)] * 2,
            pltpu.VMEM((stages * cols, side, side), jnp.float32),
            dma((2,)), dma((1,)), dma((stages,)), dma((1,)), dma((1,)), dma((1 + parts // 2,)),
            dma((1,)), dma((2,)), pltpu.SemaphoreType.REGULAR((1,)), pltpu.SemaphoreType.REGULAR((3,)),
        ],
        compiler_params=pltpu.CompilerParams(collective_id=0, has_side_effects=True, vmem_limit_bytes=48 * 2**20),
    )(slopes_in, moments_in, weights_in)


def iterate_plain(new_momentum):
    moved = lax.all_to_all(new_momentum, "fsdp", split_axis=0, concat_axis=1, tiled=True)
    gram = lax.psum(jnp.einsum("mik,mjk->mij", moved, moved, precision=HIGH), "tp")
    dot = functools.partial(jnp.einsum, "mij,mjk->mik", precision=HIGH)
    total = polynomial(gram, dot, lambda a: jnp.sum(a, axis=(1, 2), keepdims=True))
    return lax.all_to_all(dot(total, moved), "fsdp", split_axis=1, concat_axis=0, tiled=True)


def body(parts, cols, slopes_in, moments_in, weights_in):
    if slopes_in.shape[1] % 8 == 0 and parts // 4 == 2 and parts % 4 == 0:
        new_momentum, new_weights = iterate_kernel(slopes_in, moments_in, weights_in, parts, cols)
        new_weights, new_momentum = leave_kernel(new_weights, new_momentum)
    else:
        new_momentum = hold_rate * moments_in + slopes_in
        new_weights = weights_in - learn_rate * iterate_plain(new_momentum)
    return (new_weights, new_momentum)


def solution(mesh):
    return jax.shard_map(
        functools.partial(body, mesh.shape["fsdp"], mesh.shape["tp"]),
        mesh=mesh,
        in_specs=(P(None, "fsdp", "tp"), P(None, "fsdp", "tp"), P(None, "fsdp", "tp")),
        out_specs=(P(None, "fsdp", "tp"), P(None, "fsdp", "tp")),
        check_vma=False,
    )
```

```python
import functools

import jax
import jax.numpy as jnp
from jax import lax
from jax.experimental import pallas as pl
from jax.experimental.pallas import tpu as pltpu
from jax.sharding import PartitionSpec as P

ITERS = 5
HIGH = lax.Precision.HIGHEST
MESH = pl.DeviceIdType.MESH


hold_rate = 0.8
learn_rate = 1.0


def polynomial(gram, dot, trace):
    side = gram.shape[-1]
    eye = jnp.where(
        lax.broadcasted_iota(jnp.int32, (side, side), 0) == lax.broadcasted_iota(jnp.int32, (side, side), 1), 1.0, 0.0
    ).astype(gram.dtype)
    scale = lax.rsqrt(trace(gram * eye) + 1e-06)
    gram = gram * (scale * scale)
    total = None
    for step in range(ITERS):
        mixed = 3.4445 * eye - 4.775 * gram + 2.0315 * dot(gram, gram)
        total = mixed * scale if total is None else dot(mixed, total)
        if step < ITERS - 1:
            gram = dot(dot(mixed, gram), mixed)
    return total


def kernel(
    stages, parts, cols, slopes_ref, moments_ref, weights_ref, momentum_ref, new_ref,
    first_ref, sm_ref, w_ref, back_ref, x_ref, y_ref, g_ref, loads, fsend, frecv, bsend, brecv, blast, gsend, grecv, rounds,
):
    rows, wide = momentum_ref.shape[1:]
    side, mats, half, last = parts * rows, stages * parts, parts // 2, stages - 1
    f, t = lax.axis_index("fsdp"), lax.axis_index("tp")
    upper = f // half
    soon, late = (slice(None), pl.ds(0, wide // 4)), (slice(None), pl.ds(wide // 4, wide - wide // 4))

    def pair(k):
        peer = f
        for bit in range(k.bit_length()):
            if k >> bit & 1:
                peer = peer + (1 - 2 * ((f // 2**bit) % 2)) * 2**bit
        return peer

    middle = (f // 2 == half // 2 - 1) | (f // 2 == half // 2)
    outer = jnp.where(middle, 0, 1)
    first, ahead = parts - 2, first_ref.shape[1]
    known = [[], [half, half - 1, 2], [half + 1, 1], [parts - 1]]
    rest = [k for k in range(parts - 1, 0, -1) if k != first]
    inside = [pair(k) for k in range(half - 1, 0, -1)]
    outside = []
    for j in range(half // 2):
        z = upper * j + (1 - upper) * (half - 1 - j)
        x = f % 2 if j == half // 2 - 1 else 1
        outside += [2 * z + 1 - x, 2 * z + x]

    def greet(sem, *ks):
        for k in ks:
            pl.semaphore_signal(sem, inc=1, device_id={"fsdp": pair(k)}, device_id_type=MESH)

    def greet_tp(sem):
        for k in range(1, cols):
            pl.semaphore_signal(sem, inc=1, device_id={"tp": lax.rem(t + k, cols)}, device_id_type=MESH)

    barrier = pltpu.get_barrier_semaphore()

    def load_first(m, sem):
        mat = m * parts + pair(first)
        for piece in range(2):
            part = pl.ds(piece * rows // 2, rows // 2)
            pltpu.make_async_copy(slopes_ref.at[mat, part], first_ref.at[0, m, part], sem).start()
            pltpu.make_async_copy(moments_ref.at[mat, part], first_ref.at[1, m, part], sem).start()

    load_first(0, loads.at[0])
    greet(barrier, first)

    @pl.when(middle)
    def _():
        greet(barrier, 2)

    for m in range(1, ahead):
        load_first(m, loads.at[1])

    @pl.when(outer == 1)
    def _():
        greet(barrier, 1)
        greet_tp(barrier)

    def forward(m, peer):
        return pltpu.make_async_remote_copy(
            src_ref=momentum_ref.at[m * parts + peer], dst_ref=x_ref.at[m, f],
            send_sem=fsend.at[0], recv_sem=frecv.at[m],
            device_id={"fsdp": peer}, device_id_type=MESH,
        )

    def backward(m, peer, recv, *part):
        return pltpu.make_async_remote_copy(
            src_ref=y_ref.at[m, peer, *part], dst_ref=back_ref.at[m * parts + f, *part],
            send_sem=bsend.at[0], recv_sem=recv,
            device_id={"fsdp": peer}, device_id_type=MESH,
        )

    def partial(m, peer):
        return pltpu.make_async_remote_copy(
            src_ref=g_ref.at[m * cols + t], dst_ref=g_ref.at[m * cols + t],
            send_sem=gsend.at[0], recv_sem=grecv.at[lax.rem(m, 2)],
            device_id={"tp": peer}, device_id_type=MESH,
        )

    def settle(ref, sem):
        pltpu.make_async_copy(ref, ref, sem).wait()

    def add(m):
        for k in [0, *rest]:
            mat = m * parts + pair(k)
            value = hold_rate * sm_ref[1, mat] + sm_ref[0, mat]
            momentum_ref[mat] = value
            if k == 0:
                x_ref[m, f] = value

        @pl.when(m >= ahead)
        def _():
            mat = m * parts + pair(first)
            momentum_ref[mat] = hold_rate * sm_ref[1, mat] + sm_ref[0, mat]

    settle(first_ref.at[:, 0], loads.at[0])
    momentum_ref[pair(first)] = hold_rate * first_ref[1, 0] + first_ref[0, 0]
    for which, src in enumerate((slopes_ref, moments_ref)):
        pltpu.make_async_copy(src, sm_ref.at[which], loads.at[0]).start()
    pl.semaphore_wait(barrier, 1 + outer * (cols + 1))
    forward(0, pair(first)).start()
    if ahead > 1:
        settle(first_ref.at[:, pl.ds(1, ahead - 1)], loads.at[1])
    for m in range(1, ahead):
        momentum_ref[m * parts + pair(first)] = hold_rate * first_ref[1, m] + first_ref[0, m]
        forward(m, pair(first)).start()

    @pl.when(outer == 1)
    def _():
        greet(rounds.at[0], 2, 1, first)
        greet_tp(rounds.at[0])

    settle(sm_ref, loads.at[0])

    @pl.loop(0, stages)
    def _(m):
        add(m)

    weights = pltpu.make_async_copy(weights_ref, w_ref, loads.at[1])
    weights.start()

    pl.semaphore_wait(rounds.at[0], 1 + outer * cols)

    @pl.when(outer == 1)
    def _():
        greet(rounds.at[1], 2, 1, first)

    for k in known[1]:
        forward(0, pair(k)).start()
    pl.semaphore_wait(rounds.at[1], 1 + outer)

    @pl.when(outer == 1)
    def _():
        greet(rounds.at[2], 2)

    for k in known[2]:
        forward(0, pair(k)).start()

    @pl.when(middle)
    def _():
        pl.semaphore_wait(rounds.at[2], 1)

    for k in known[3]:
        forward(0, pair(k)).start()

    @pl.loop(1, stages)
    def _(m):
        for k in rest:
            forward(m, pair(k)).start()

        @pl.when(m >= ahead)
        def _():
            forward(m, pair(first)).start()

    dot = functools.partial(jnp.dot, precision=HIGH, preferred_element_type=jnp.float32)

    @pl.loop(0, stages)
    def _(m):
        settle(x_ref.at[m, pl.ds(0, parts - 1)], frecv.at[m])
        x = x_ref[m].reshape(side, wide)
        g_ref[m * cols + t] = lax.dot_general(x, x, (((1,), (1,)), ((), ())), precision=HIGH, preferred_element_type=jnp.float32)
        for k in range(1, cols):
            partial(m, lax.rem(t + k, cols)).start()
        settle(g_ref.at[pl.ds(m * cols, cols - 1)], grecv.at[lax.rem(m, 2)])
        gram = g_ref[m * cols]
        for k in range(1, cols):
            gram = gram + g_ref[m * cols + k]
        total = polynomial(gram, dot, lambda a: jnp.sum(jnp.sum(a, axis=1, keepdims=True), axis=0, keepdims=True))
        y_ref[m] = dot(total, x_ref[m].reshape(side, wide)).reshape(parts, rows, wide)

        @pl.when(m < last)
        def _():
            for peer in outside[:-1] + inside:
                backward(m, peer, brecv.at[0]).start()

        @pl.when(m < last - 1)
        def _():
            backward(m, outside[-1], brecv.at[0]).start()

        @pl.when(m == last)
        def _():
            for peer in inside:
                backward(m, peer, brecv.at[0]).start()
            backward(m, outside[0], blast.at[f % half]).start()
            for peer in outside[1:-1]:
                backward(m, peer, blast.at[f % half]).start()
            if last:
                backward(last - 1, outside[-1], brecv.at[0]).start()

            backward(m, outside[-1], blast.at[f % half], *soon).start()

            @pl.when(t % 2 == 0)
            def _():
                backward(m, outside[-1], blast.at[f % half], *late).start()

    def finish(m, peers):
        for peer in peers:
            mat = m * parts + peer
            new_ref[mat] = w_ref[mat] - learn_rate * back_ref[mat]

    weights.wait()
    for m in range(stages):
        new_ref[m * parts + f] = w_ref[m * parts + f] - learn_rate * y_ref[m, f]
    @pl.when(t % 2 == 1)
    def _():
        settle(back_ref.at[pl.ds(0, mats - stages - 1)], bsend.at[0])
        backward(last, outside[-1], blast.at[f % half], *late).start()

    settle(back_ref.at[pl.ds(0, last * (parts - 1) + len(inside))], brecv.at[0])
    finish(last, inside)

    @pl.loop(0, last)
    def _(m):
        finish(m, inside + outside)

    for peer in outside:
        settle(back_ref.at[last * parts + peer], blast.at[peer % half])
        finish(last, [peer])

    settle(momentum_ref.at[pl.ds(0, mats - stages)], fsend.at[0])
    @pl.when(t % 2 == 1)
    def _():
        settle(back_ref.at[pl.ds(0, 1)], bsend.at[0])

    @pl.when(t % 2 == 0)
    def _():
        settle(back_ref.at[pl.ds(0, mats - stages)], bsend.at[0])

    settle(g_ref.at[pl.ds(0, stages * (cols - 1))], gsend.at[0])


def leave(first_ref, second_ref, first_out, second_out, sems):
    copies = [pltpu.make_async_copy(first_ref, first_out, sems.at[0]), pltpu.make_async_copy(second_ref, second_out, sems.at[1])]
    for copy in copies:
        copy.start()
    for copy in copies:
        copy.wait()


def leave_kernel(first, second):
    return pl.pallas_call(
        leave,
        out_shape=[jax.ShapeDtypeStruct(a.shape, a.dtype) for a in (first, second)],
        in_specs=[pl.BlockSpec(memory_space=pl.ANY)] * 2,
        out_specs=[pl.BlockSpec(memory_space=pl.ANY)] * 2,
        scratch_shapes=[pltpu.SemaphoreType.DMA((2,))],
        compiler_params=pltpu.CompilerParams(vmem_limit_bytes=2**20),
    )(first, second)


def iterate_kernel(slopes_in, moments_in, weights_in, parts, cols):
    mats, rows, wide = slopes_in.shape
    stages, side = mats // parts, rows * parts
    dma = pltpu.SemaphoreType.DMA
    ahead = (stages + 1) // 2
    return pl.pallas_call(
        functools.partial(kernel, stages, parts, cols),
        out_shape=[jax.ShapeDtypeStruct(slopes_in.shape, slopes_in.dtype)] * 2,
        in_specs=[pl.BlockSpec(memory_space=pltpu.HBM)] * 3,
        out_specs=[pl.BlockSpec(memory_space=pltpu.VMEM)] * 2,
        scratch_shapes=[
            pltpu.VMEM((2, ahead, rows, wide), jnp.float32),
            pltpu.VMEM((2, mats, rows, wide), jnp.float32),
            *[pltpu.VMEM((mats, rows, wide), jnp.float32)] * 2,
            *[pltpu.VMEM((stages, parts, rows, wide), jnp.float32)] * 2,
            pltpu.VMEM((stages * cols, side, side), jnp.float32),
            dma((2,)), dma((1,)), dma((stages,)), dma((1,)), dma((1,)), dma((parts // 2,)),
            dma((1,)), dma((2,)), pltpu.SemaphoreType.REGULAR((3,)),
        ],
        compiler_params=pltpu.CompilerParams(collective_id=0, has_side_effects=True, vmem_limit_bytes=48 * 2**20),
    )(slopes_in, moments_in, weights_in)


def iterate_plain(new_momentum):
    moved = lax.all_to_all(new_momentum, "fsdp", split_axis=0, concat_axis=1, tiled=True)
    gram = lax.psum(jnp.einsum("mik,mjk->mij", moved, moved, precision=HIGH), "tp")
    dot = functools.partial(jnp.einsum, "mij,mjk->mik", precision=HIGH)
    total = polynomial(gram, dot, lambda a: jnp.sum(a, axis=(1, 2), keepdims=True))
    return lax.all_to_all(dot(total, moved), "fsdp", split_axis=1, concat_axis=0, tiled=True)


def body(parts, cols, slopes_in, moments_in, weights_in):
    if slopes_in.shape[1] % 8 == 0 and parts // 4 == 2 and parts % 4 == 0:
        new_momentum, new_weights = iterate_kernel(slopes_in, moments_in, weights_in, parts, cols)
        new_weights, new_momentum = leave_kernel(new_weights, new_momentum)
    else:
        new_momentum = hold_rate * moments_in + slopes_in
        new_weights = weights_in - learn_rate * iterate_plain(new_momentum)
    return (new_weights, new_momentum)


def solution(mesh):
    return jax.shard_map(
        functools.partial(body, mesh.shape["fsdp"], mesh.shape["tp"]),
        mesh=mesh,
        in_specs=(P(None, "fsdp", "tp"), P(None, "fsdp", "tp"), P(None, "fsdp", "tp")),
        out_specs=(P(None, "fsdp", "tp"), P(None, "fsdp", "tp")),
        check_vma=False,
    )
```

```python
import functools

import jax
import jax.numpy as jnp
from jax import lax
from jax.experimental import pallas as pl
from jax.experimental.pallas import tpu as pltpu
from jax.sharding import PartitionSpec as P

ITERS = 5
HIGH = lax.Precision.HIGHEST
MESH = pl.DeviceIdType.MESH


hold_rate = 0.8
learn_rate = 1.0


def polynomial(gram, dot, trace):
    side = gram.shape[-1]
    eye = jnp.where(
        lax.broadcasted_iota(jnp.int32, (side, side), 0) == lax.broadcasted_iota(jnp.int32, (side, side), 1), 1.0, 0.0
    ).astype(gram.dtype)
    scale = lax.rsqrt(trace(gram * eye) + 1e-06)
    gram = gram * (scale * scale)
    total = None
    for step in range(ITERS):
        mixed = 3.4445 * eye - 4.775 * gram + 2.0315 * dot(gram, gram)
        total = mixed * scale if total is None else dot(mixed, total)
        if step < ITERS - 1:
            gram = dot(dot(mixed, gram), mixed)
    return total


def kernel(
    stages, parts, cols, slopes_ref, moments_ref, weights_ref, momentum_ref, new_ref,
    first_ref, sm_ref, w_ref, back_ref, x_ref, y_ref, g_ref, loads, fsend, frecv, bsend, brecv, blast, gsend, grecv, rounds,
):
    rows, wide = momentum_ref.shape[1:]
    side, mats, half, last = parts * rows, stages * parts, parts // 2, stages - 1
    f, t = lax.axis_index("fsdp"), lax.axis_index("tp")
    upper = f // half
    soon, late = (slice(None), pl.ds(0, wide // 4)), (slice(None), pl.ds(wide // 4, wide - wide // 4))

    def pair(k):
        peer = f
        for bit in range(k.bit_length()):
            if k >> bit & 1:
                peer = peer + (1 - 2 * ((f // 2**bit) % 2)) * 2**bit
        return peer

    middle = (f // 2 == half // 2 - 1) | (f // 2 == half // 2)
    outer = jnp.where(middle, 0, 1)
    first, ahead = parts - 2, first_ref.shape[1]
    known = [[], [half, half - 1, 2], [half + 1, 1], [parts - 1]]
    rest = [k for k in range(parts - 1, 0, -1) if k != first]
    inside = [pair(k) for k in range(half - 1, 0, -1)]
    outside = []
    for j in range(half // 2):
        z = upper * j + (1 - upper) * (half - 1 - j)
        x = f % 2 if j == half // 2 - 1 else 1
        outside += [2 * z + 1 - x, 2 * z + x]

    def greet(sem, *ks):
        for k in ks:
            pl.semaphore_signal(sem, inc=1, device_id={"fsdp": pair(k)}, device_id_type=MESH)

    def greet_tp(sem):
        for k in range(1, cols):
            pl.semaphore_signal(sem, inc=1, device_id={"tp": lax.rem(t + k, cols)}, device_id_type=MESH)

    barrier = pltpu.get_barrier_semaphore()

    def load_first(m, sem):
        mat = m * parts + pair(first)
        for piece in range(2):
            part = pl.ds(piece * rows // 2, rows // 2)
            pltpu.make_async_copy(slopes_ref.at[mat, part], first_ref.at[0, m, part], sem).start()
            pltpu.make_async_copy(moments_ref.at[mat, part], first_ref.at[1, m, part], sem).start()

    load_first(0, loads.at[0])
    greet(barrier, first)

    @pl.when(middle)
    def _():
        greet(barrier, 2)

    for m in range(1, ahead):
        load_first(m, loads.at[1])

    @pl.when(outer == 1)
    def _():
        greet(barrier, 1)
        greet_tp(barrier)

    def forward(m, peer):
        return pltpu.make_async_remote_copy(
            src_ref=momentum_ref.at[m * parts + peer], dst_ref=x_ref.at[m, f],
            send_sem=fsend.at[0], recv_sem=frecv.at[m],
            device_id={"fsdp": peer}, device_id_type=MESH,
        )

    def backward(m, peer, recv, *part):
        return pltpu.make_async_remote_copy(
            src_ref=y_ref.at[m, peer, *part], dst_ref=back_ref.at[m * parts + f, *part],
            send_sem=bsend.at[0], recv_sem=recv,
            device_id={"fsdp": peer}, device_id_type=MESH,
        )

    def partial(m, peer):
        return pltpu.make_async_remote_copy(
            src_ref=g_ref.at[m * cols + t], dst_ref=g_ref.at[m * cols + t],
            send_sem=gsend.at[0], recv_sem=grecv.at[lax.rem(m, 2)],
            device_id={"tp": peer}, device_id_type=MESH,
        )

    def settle(ref, sem):
        pltpu.make_async_copy(ref, ref, sem).wait()

    def add(m):
        for k in [0, *rest]:
            mat = m * parts + pair(k)
            value = hold_rate * sm_ref[1, mat] + sm_ref[0, mat]
            momentum_ref[mat] = value
            if k == 0:
                x_ref[m, f] = value

        @pl.when(m >= ahead)
        def _():
            mat = m * parts + pair(first)
            momentum_ref[mat] = hold_rate * sm_ref[1, mat] + sm_ref[0, mat]

    settle(first_ref.at[:, 0], loads.at[0])
    momentum_ref[pair(first)] = hold_rate * first_ref[1, 0] + first_ref[0, 0]
    for which, src in enumerate((slopes_ref, moments_ref)):
        pltpu.make_async_copy(src, sm_ref.at[which], loads.at[0]).start()
    pl.semaphore_wait(barrier, 1 + outer * (cols + 1))
    forward(0, pair(first)).start()
    if ahead > 1:
        settle(first_ref.at[:, pl.ds(1, ahead - 1)], loads.at[1])
    for m in range(1, ahead):
        momentum_ref[m * parts + pair(first)] = hold_rate * first_ref[1, m] + first_ref[0, m]
        forward(m, pair(first)).start()

    @pl.when(outer == 1)
    def _():
        greet(rounds.at[0], 2, 1, first)
        greet_tp(rounds.at[0])

    settle(sm_ref, loads.at[0])

    @pl.loop(0, stages)
    def _(m):
        add(m)

    weights = pltpu.make_async_copy(weights_ref, w_ref, loads.at[1])
    weights.start()

    pl.semaphore_wait(rounds.at[0], 1 + outer * cols)

    @pl.when(outer == 1)
    def _():
        greet(rounds.at[1], 2, 1, first)

    for k in known[1]:
        forward(0, pair(k)).start()
    pl.semaphore_wait(rounds.at[1], 1 + outer)

    @pl.when(outer == 1)
    def _():
        greet(rounds.at[2], 2)

    for k in known[2]:
        forward(0, pair(k)).start()

    @pl.when(middle)
    def _():
        pl.semaphore_wait(rounds.at[2], 1)

    for k in known[3]:
        forward(0, pair(k)).start()

    @pl.loop(1, stages)
    def _(m):
        for k in rest:
            forward(m, pair(k)).start()

        @pl.when(m >= ahead)
        def _():
            forward(m, pair(first)).start()

    dot = functools.partial(jnp.dot, precision=HIGH, preferred_element_type=jnp.float32)

    @pl.loop(0, stages)
    def _(m):
        settle(x_ref.at[m, pl.ds(0, parts - 1)], frecv.at[m])
        x = x_ref[m].reshape(side, wide)
        g_ref[m * cols + t] = lax.dot_general(x, x, (((1,), (1,)), ((), ())), precision=HIGH, preferred_element_type=jnp.float32)
        for k in range(1, cols):
            partial(m, lax.rem(t + k, cols)).start()
        settle(g_ref.at[pl.ds(m * cols, cols - 1)], grecv.at[lax.rem(m, 2)])
        gram = g_ref[m * cols]
        for k in range(1, cols):
            gram = gram + g_ref[m * cols + k]
        total = polynomial(gram, dot, lambda a: jnp.sum(jnp.sum(a, axis=1, keepdims=True), axis=0, keepdims=True))
        y_ref[m] = dot(total, x_ref[m].reshape(side, wide)).reshape(parts, rows, wide)

        @pl.when(m < last)
        def _():
            for peer in outside[:-1] + inside:
                backward(m, peer, brecv.at[0]).start()

        @pl.when(m < last - 1)
        def _():
            backward(m, outside[-1], brecv.at[0]).start()

        @pl.when(m == last)
        def _():
            for peer in inside:
                backward(m, peer, brecv.at[0]).start()
            backward(m, outside[0], blast.at[f % half]).start()
            for peer in outside[1:-1]:
                backward(m, peer, blast.at[f % half]).start()
            if last:
                backward(last - 1, outside[-1], brecv.at[0]).start()

            backward(m, outside[-1], blast.at[f % half], *soon).start()

            @pl.when(t % 2 == 0)
            def _():
                backward(m, outside[-1], blast.at[f % half], *late).start()

    def finish(m, peers):
        for peer in peers:
            mat = m * parts + peer
            new_ref[mat] = w_ref[mat] - learn_rate * back_ref[mat]

    weights.wait()
    for m in range(stages):
        new_ref[m * parts + f] = w_ref[m * parts + f] - learn_rate * y_ref[m, f]
    @pl.when(t % 2 == 1)
    def _():
        settle(back_ref.at[pl.ds(0, mats - stages - 1)], bsend.at[0])
        backward(last, outside[-1], blast.at[f % half], *late).start()

    settle(momentum_ref.at[pl.ds(0, mats - stages)], fsend.at[0])
    settle(g_ref.at[pl.ds(0, stages * (cols - 1))], gsend.at[0])
    settle(back_ref.at[pl.ds(0, last * (parts - 1) + len(inside))], brecv.at[0])
    finish(last, inside)

    @pl.loop(0, last)
    def _(m):
        finish(m, inside + outside)

    for peer in outside:
        settle(back_ref.at[last * parts + peer], blast.at[peer % half])
        finish(last, [peer])

    @pl.when(t % 2 == 1)
    def _():
        settle(back_ref.at[pl.ds(0, 1)], bsend.at[0])

    @pl.when(t % 2 == 0)
    def _():
        settle(back_ref.at[pl.ds(0, mats - stages)], bsend.at[0])


def leave(first_ref, second_ref, first_out, second_out, sems):
    copies = [pltpu.make_async_copy(first_ref, first_out, sems.at[0]), pltpu.make_async_copy(second_ref, second_out, sems.at[1])]
    for copy in copies:
        copy.start()
    for copy in copies:
        copy.wait()


def leave_kernel(first, second):
    return pl.pallas_call(
        leave,
        out_shape=[jax.ShapeDtypeStruct(a.shape, a.dtype) for a in (first, second)],
        in_specs=[pl.BlockSpec(memory_space=pl.ANY)] * 2,
        out_specs=[pl.BlockSpec(memory_space=pl.ANY)] * 2,
        scratch_shapes=[pltpu.SemaphoreType.DMA((2,))],
        compiler_params=pltpu.CompilerParams(vmem_limit_bytes=2**20),
    )(first, second)


def iterate_kernel(slopes_in, moments_in, weights_in, parts, cols):
    mats, rows, wide = slopes_in.shape
    stages, side = mats // parts, rows * parts
    dma = pltpu.SemaphoreType.DMA
    ahead = (stages + 1) // 2
    return pl.pallas_call(
        functools.partial(kernel, stages, parts, cols),
        out_shape=[jax.ShapeDtypeStruct(slopes_in.shape, slopes_in.dtype)] * 2,
        in_specs=[pl.BlockSpec(memory_space=pltpu.HBM)] * 3,
        out_specs=[pl.BlockSpec(memory_space=pltpu.VMEM)] * 2,
        scratch_shapes=[
            pltpu.VMEM((2, ahead, rows, wide), jnp.float32),
            pltpu.VMEM((2, mats, rows, wide), jnp.float32),
            *[pltpu.VMEM((mats, rows, wide), jnp.float32)] * 2,
            *[pltpu.VMEM((stages, parts, rows, wide), jnp.float32)] * 2,
            pltpu.VMEM((stages * cols, side, side), jnp.float32),
            dma((2,)), dma((1,)), dma((stages,)), dma((1,)), dma((1,)), dma((parts // 2,)),
            dma((1,)), dma((2,)), pltpu.SemaphoreType.REGULAR((3,)),
        ],
        compiler_params=pltpu.CompilerParams(collective_id=0, has_side_effects=True, vmem_limit_bytes=48 * 2**20),
    )(slopes_in, moments_in, weights_in)


def iterate_plain(new_momentum):
    moved = lax.all_to_all(new_momentum, "fsdp", split_axis=0, concat_axis=1, tiled=True)
    gram = lax.psum(jnp.einsum("mik,mjk->mij", moved, moved, precision=HIGH), "tp")
    dot = functools.partial(jnp.einsum, "mij,mjk->mik", precision=HIGH)
    total = polynomial(gram, dot, lambda a: jnp.sum(a, axis=(1, 2), keepdims=True))
    return lax.all_to_all(dot(total, moved), "fsdp", split_axis=1, concat_axis=0, tiled=True)


def body(parts, cols, slopes_in, moments_in, weights_in):
    if slopes_in.shape[1] % 8 == 0 and parts // 4 == 2 and parts % 4 == 0:
        new_momentum, new_weights = iterate_kernel(slopes_in, moments_in, weights_in, parts, cols)
        new_weights, new_momentum = leave_kernel(new_weights, new_momentum)
    else:
        new_momentum = hold_rate * moments_in + slopes_in
        new_weights = weights_in - learn_rate * iterate_plain(new_momentum)
    return (new_weights, new_momentum)


def solution(mesh):
    return jax.shard_map(
        functools.partial(body, mesh.shape["fsdp"], mesh.shape["tp"]),
        mesh=mesh,
        in_specs=(P(None, "fsdp", "tp"), P(None, "fsdp", "tp"), P(None, "fsdp", "tp")),
        out_specs=(P(None, "fsdp", "tp"), P(None, "fsdp", "tp")),
        check_vma=False,
    )
```

```python
import functools

import jax
import jax.numpy as jnp
from jax import lax
from jax.experimental import pallas as pl
from jax.experimental.pallas import tpu as pltpu
from jax.sharding import PartitionSpec as P

ITERS = 5
HIGH = lax.Precision.HIGHEST
MESH = pl.DeviceIdType.MESH


hold_rate = 0.8
learn_rate = 1.0


def polynomial(gram, dot, trace):
    side = gram.shape[-1]
    eye = jnp.where(
        lax.broadcasted_iota(jnp.int32, (side, side), 0) == lax.broadcasted_iota(jnp.int32, (side, side), 1), 1.0, 0.0
    ).astype(gram.dtype)
    scale = lax.rsqrt(trace(gram * eye) + 1e-06)
    gram = gram * (scale * scale)
    total = None
    for step in range(ITERS):
        mixed = 3.4445 * eye - 4.775 * gram + 2.0315 * dot(gram, gram)
        total = mixed * scale if total is None else dot(mixed, total)
        if step < ITERS - 1:
            gram = dot(dot(mixed, gram), mixed)
    return total


def kernel(
    stages, parts, cols, slopes_ref, moments_ref, weights_ref, momentum_ref, new_ref,
    first_ref, sm_ref, w_ref, back_ref, x_ref, y_ref, g_ref, loads, fsend, frecv, bsend, brecv, blast, gsend, grecv, rounds,
):
    rows, wide = momentum_ref.shape[1:]
    side, mats, half, last = parts * rows, stages * parts, parts // 2, stages - 1
    f, t = lax.axis_index("fsdp"), lax.axis_index("tp")
    upper = f // half
    soon, late = (slice(None), pl.ds(0, wide // 4)), (slice(None), pl.ds(wide // 4, wide - wide // 4))

    def pair(k):
        peer = f
        for bit in range(k.bit_length()):
            if k >> bit & 1:
                peer = peer + (1 - 2 * ((f // 2**bit) % 2)) * 2**bit
        return peer

    middle = (f // 2 == half // 2 - 1) | (f // 2 == half // 2)
    outer = jnp.where(middle, 0, 1)
    mine = (1 - outer) * (1 + f % 2)
    first, ahead = parts - 2, first_ref.shape[1]
    known = [[], [half, half - 1, 2], [half + 1, 1], [parts - 1]]
    rest = [k for k in range(parts - 1, 0, -1) if k != first]
    inside = [pair(k) for k in range(half - 1, 0, -1)]
    outside = []
    for j in range(half // 2):
        z = upper * j + (1 - upper) * (half - 1 - j)
        x = f % 2 if j == half // 2 - 1 else 1
        outside += [2 * z + 1 - x, 2 * z + x]

    def greet(sem, *ks):
        for k in ks:
            pl.semaphore_signal(sem, inc=1, device_id={"fsdp": pair(k)}, device_id_type=MESH)

    def greet_tp(sem):
        for k in range(1, cols):
            pl.semaphore_signal(sem, inc=1, device_id={"tp": lax.rem(t + k, cols)}, device_id_type=MESH)

    barrier = pltpu.get_barrier_semaphore()

    def load_first(m, sem):
        mat = m * parts + pair(first)
        for piece in range(2):
            part = pl.ds(piece * rows // 2, rows // 2)
            pltpu.make_async_copy(slopes_ref.at[mat, part], first_ref.at[0, m, part], sem).start()
            pltpu.make_async_copy(moments_ref.at[mat, part], first_ref.at[1, m, part], sem).start()

    load_first(0, loads.at[0])
    greet(barrier, first)

    @pl.when(middle)
    def _():
        greet(barrier, 2)

    for m in range(1, ahead):
        load_first(m, loads.at[1])

    @pl.when(outer == 1)
    def _():
        greet(barrier, 1)
        greet_tp(barrier)

    def forward(m, peer):
        return pltpu.make_async_remote_copy(
            src_ref=momentum_ref.at[m * parts + peer], dst_ref=x_ref.at[m, f],
            send_sem=fsend.at[0], recv_sem=frecv.at[m],
            device_id={"fsdp": peer}, device_id_type=MESH,
        )

    def backward(m, peer, recv, *part):
        return pltpu.make_async_remote_copy(
            src_ref=y_ref.at[m, peer, *part], dst_ref=back_ref.at[m * parts + f, *part],
            send_sem=bsend.at[0], recv_sem=recv,
            device_id={"fsdp": peer}, device_id_type=MESH,
        )

    def partial(m, peer):
        return pltpu.make_async_remote_copy(
            src_ref=g_ref.at[m * cols + t], dst_ref=g_ref.at[m * cols + t],
            send_sem=gsend.at[0], recv_sem=grecv.at[lax.rem(m, 2)],
            device_id={"tp": peer}, device_id_type=MESH,
        )

    def settle(ref, sem):
        pltpu.make_async_copy(ref, ref, sem).wait()

    def add(m):
        for k in [0, *rest]:
            mat = m * parts + pair(k)
            value = hold_rate * sm_ref[1, mat] + sm_ref[0, mat]
            momentum_ref[mat] = value
            if k == 0:
                x_ref[m, f] = value

        @pl.when(m >= ahead)
        def _():
            mat = m * parts + pair(first)
            momentum_ref[mat] = hold_rate * sm_ref[1, mat] + sm_ref[0, mat]

    settle(first_ref.at[:, 0], loads.at[0])
    momentum_ref[pair(first)] = hold_rate * first_ref[1, 0] + first_ref[0, 0]
    for which, src in enumerate((slopes_ref, moments_ref)):
        pltpu.make_async_copy(src, sm_ref.at[which], loads.at[0]).start()
    pl.semaphore_wait(barrier, 1 + outer * (cols + 1))
    forward(0, pair(first)).start()
    if ahead > 1:
        settle(first_ref.at[:, pl.ds(1, ahead - 1)], loads.at[1])
    for m in range(1, ahead):
        momentum_ref[m * parts + pair(first)] = hold_rate * first_ref[1, m] + first_ref[0, m]
        forward(m, pair(first)).start()

    @pl.when(outer == 1)
    def _():
        greet(rounds.at[0], 2, 1, first)
        greet_tp(rounds.at[0])

    settle(sm_ref, loads.at[0])

    @pl.loop(0, stages)
    def _(m):
        add(m)

    weights = pltpu.make_async_copy(weights_ref, w_ref, loads.at[1])
    weights.start()

    pl.semaphore_wait(rounds.at[0], 1 + outer * cols)

    @pl.when(outer == 1)
    def _():
        greet(rounds.at[1], 2, 1, first)

    for k in known[1]:
        forward(0, pair(k)).start()
    pl.semaphore_wait(rounds.at[1], 1 + outer)

    @pl.when(outer == 1)
    def _():
        greet(rounds.at[2], 2)

    for k in known[2]:
        forward(0, pair(k)).start()

    @pl.when(middle)
    def _():
        pl.semaphore_wait(rounds.at[2], 1)

    for k in known[3]:
        forward(0, pair(k)).start()

    @pl.loop(1, stages)
    def _(m):
        for k in rest:
            forward(m, pair(k)).start()

        @pl.when(m >= ahead)
        def _():
            forward(m, pair(first)).start()

    dot = functools.partial(jnp.dot, precision=HIGH, preferred_element_type=jnp.float32)

    @pl.loop(0, stages)
    def _(m):
        settle(x_ref.at[m, pl.ds(0, parts - 1)], frecv.at[m])
        x = x_ref[m].reshape(side, wide)
        g_ref[m * cols + t] = lax.dot_general(x, x, (((1,), (1,)), ((), ())), precision=HIGH, preferred_element_type=jnp.float32)
        for k in range(1, cols):
            partial(m, lax.rem(t + k, cols)).start()
        settle(g_ref.at[pl.ds(m * cols, cols - 1)], grecv.at[lax.rem(m, 2)])
        gram = g_ref[m * cols]
        for k in range(1, cols):
            gram = gram + g_ref[m * cols + k]
        total = polynomial(gram, dot, lambda a: jnp.sum(jnp.sum(a, axis=1, keepdims=True), axis=0, keepdims=True))
        y_ref[m] = dot(total, x_ref[m].reshape(side, wide)).reshape(parts, rows, wide)

        @pl.when(m < last)
        def _():
            for peer in outside[:-1] + inside:
                backward(m, peer, brecv.at[0]).start()

        @pl.when(m < last - 1)
        def _():
            backward(m, outside[-1], brecv.at[0]).start()

        @pl.when(m == last)
        def _():
            for peer in inside:
                backward(m, peer, brecv.at[0]).start()
            backward(m, outside[0], blast.at[mine]).start()
            for peer in outside[1:-1]:
                backward(m, peer, blast.at[mine]).start()
            if last:
                backward(last - 1, outside[-1], brecv.at[0]).start()

            backward(m, outside[-1], blast.at[mine], *soon).start()

            @pl.when(t % 2 == 0)
            def _():
                backward(m, outside[-1], blast.at[mine], *late).start()

    def finish(m, peers):
        for peer in peers:
            mat = m * parts + peer
            new_ref[mat] = w_ref[mat] - learn_rate * back_ref[mat]

    weights.wait()
    for m in range(stages):
        new_ref[m * parts + f] = w_ref[m * parts + f] - learn_rate * y_ref[m, f]
    @pl.when(t % 2 == 1)
    def _():
        settle(back_ref.at[pl.ds(0, mats - stages - 1)], bsend.at[0])
        backward(last, outside[-1], blast.at[mine], *late).start()

    settle(momentum_ref.at[pl.ds(0, mats - stages)], fsend.at[0])
    settle(g_ref.at[pl.ds(0, stages * (cols - 1))], gsend.at[0])
    settle(back_ref.at[pl.ds(0, last * (parts - 1) + len(inside))], brecv.at[0])
    finish(last, inside)

    @pl.loop(0, last)
    def _(m):
        finish(m, inside + outside)

    settle(back_ref.at[pl.ds(0, 2)], blast.at[0])
    finish(last, outside[:2])
    for peer in outside[2:]:
        settle(back_ref.at[last * parts + peer], blast.at[1 + peer % 2])
        finish(last, [peer])

    @pl.when(t % 2 == 1)
    def _():
        settle(back_ref.at[pl.ds(0, 1)], bsend.at[0])

    @pl.when(t % 2 == 0)
    def _():
        settle(back_ref.at[pl.ds(0, mats - stages)], bsend.at[0])


def leave(first_ref, second_ref, first_out, second_out, sems):
    copies = [pltpu.make_async_copy(first_ref, first_out, sems.at[0]), pltpu.make_async_copy(second_ref, second_out, sems.at[1])]
    for copy in copies:
        copy.start()
    for copy in copies:
        copy.wait()


def leave_kernel(first, second):
    return pl.pallas_call(
        leave,
        out_shape=[jax.ShapeDtypeStruct(a.shape, a.dtype) for a in (first, second)],
        in_specs=[pl.BlockSpec(memory_space=pl.ANY)] * 2,
        out_specs=[pl.BlockSpec(memory_space=pl.ANY)] * 2,
        scratch_shapes=[pltpu.SemaphoreType.DMA((2,))],
        compiler_params=pltpu.CompilerParams(vmem_limit_bytes=2**20),
    )(first, second)


def iterate_kernel(slopes_in, moments_in, weights_in, parts, cols):
    mats, rows, wide = slopes_in.shape
    stages, side = mats // parts, rows * parts
    dma = pltpu.SemaphoreType.DMA
    ahead = (stages + 1) // 2
    return pl.pallas_call(
        functools.partial(kernel, stages, parts, cols),
        out_shape=[jax.ShapeDtypeStruct(slopes_in.shape, slopes_in.dtype)] * 2,
        in_specs=[pl.BlockSpec(memory_space=pltpu.HBM)] * 3,
        out_specs=[pl.BlockSpec(memory_space=pltpu.VMEM)] * 2,
        scratch_shapes=[
            pltpu.VMEM((2, ahead, rows, wide), jnp.float32),
            pltpu.VMEM((2, mats, rows, wide), jnp.float32),
            *[pltpu.VMEM((mats, rows, wide), jnp.float32)] * 2,
            *[pltpu.VMEM((stages, parts, rows, wide), jnp.float32)] * 2,
            pltpu.VMEM((stages * cols, side, side), jnp.float32),
            dma((2,)), dma((1,)), dma((stages,)), dma((1,)), dma((1,)), dma((3,)),
            dma((1,)), dma((2,)), pltpu.SemaphoreType.REGULAR((3,)),
        ],
        compiler_params=pltpu.CompilerParams(collective_id=0, has_side_effects=True, vmem_limit_bytes=48 * 2**20),
    )(slopes_in, moments_in, weights_in)


def iterate_plain(new_momentum):
    moved = lax.all_to_all(new_momentum, "fsdp", split_axis=0, concat_axis=1, tiled=True)
    gram = lax.psum(jnp.einsum("mik,mjk->mij", moved, moved, precision=HIGH), "tp")
    dot = functools.partial(jnp.einsum, "mij,mjk->mik", precision=HIGH)
    total = polynomial(gram, dot, lambda a: jnp.sum(a, axis=(1, 2), keepdims=True))
    return lax.all_to_all(dot(total, moved), "fsdp", split_axis=1, concat_axis=0, tiled=True)


def body(parts, cols, slopes_in, moments_in, weights_in):
    if slopes_in.shape[1] % 8 == 0 and parts // 4 == 2 and parts % 4 == 0:
        new_momentum, new_weights = iterate_kernel(slopes_in, moments_in, weights_in, parts, cols)
        new_weights, new_momentum = leave_kernel(new_weights, new_momentum)
    else:
        new_momentum = hold_rate * moments_in + slopes_in
        new_weights = weights_in - learn_rate * iterate_plain(new_momentum)
    return (new_weights, new_momentum)


def solution(mesh):
    return jax.shard_map(
        functools.partial(body, mesh.shape["fsdp"], mesh.shape["tp"]),
        mesh=mesh,
        in_specs=(P(None, "fsdp", "tp"), P(None, "fsdp", "tp"), P(None, "fsdp", "tp")),
        out_specs=(P(None, "fsdp", "tp"), P(None, "fsdp", "tp")),
        check_vma=False,
    )
```
